128 devices in a mesh: outer: 8 (over z, y_lo), inner: 16 (over y_hi, x, core).
Axes of the slice: x: 4, y: 4 (y_hi: 2, y_lo: 2; y = y_hi * 2 + y_lo), z: 4, core: 2. Of those that a mesh axis runs over, the one named last changes fastest.
Arguments:
- query_gate: bfloat16 [4096, 16384], P(None, ('outer', 'inner')), may hold values from -6 to 6
- key_proj: bfloat16 [4096, 16384], P(None, ('outer', 'inner')), may hold values from -6 to 6
- value_proj: bfloat16 [4096, 16384], P(None, ('outer', 'inner')), may hold values from -6 to 6
- out_grad: bfloat16 [4096, 16384], P(None, ('outer', 'inner')), may hold values from -6 to 6
- filters: float32 [4096, 16384], P(None, ('outer', 'inner')), may hold values from -8 to 8
- skip_bias: float32 [4096], P(('outer', 'inner')), may hold values from -4 to 4
Outputs:
- output: bfloat16 [4096, 16384], P(None, ('outer', 'inner'))
- query_grad: bfloat16 [4096, 16384], P(None, ('outer', 'inner'))
- key_grad: bfloat16 [4096, 16384], P(None, ('outer', 'inner'))
- value_grad: bfloat16 [4096, 16384], P(None, ('outer', 'inner'))
- filter_grad: float32 [4096, 16384], P(None, ('outer', 'inner'))
- bias_grad: float32 [4096], P(('outer', 'inner'))
The draws below stay inside these ranges and needn't reach their ends.
All inputs are finite; a program needn't handle non-finite values.
Results may differ from the reference program's by a relative error of at most 0.0058.
Values may be sent and summed in bfloat16 or wider, within the bound.
A program may use at most 128 MiB of HBM per device.

```python
import math
import jax
import jax.numpy as jnp
from jax import lax

D = 4096
SEQUENCE_LENGTH = 16384


def draw_filters(key, part):
    jitter_random_key, variety_random_key, quick_random_key, gradual_random_key, spike_random_key, scale_random_key = jax.random.split(key, 6)
    noise_vals = jnp.clip(jax.random.normal(jitter_random_key, (D, SEQUENCE_LENGTH), jnp.float32), -4.0, 4.0)
    kind_draw = jax.random.randint(variety_random_key, (D, 1), 0, 10)
    position_index = jnp.arange(SEQUENCE_LENGTH, dtype=jnp.float32)[None, :]
    fast_decay = jnp.exp(jax.random.uniform(quick_random_key, (D, 1), jnp.float32, math.log(10.0), math.log(20.0)))
    slow_decay = jnp.exp(jax.random.uniform(gradual_random_key, (D, 1), jnp.float32, math.log(2.0 * SEQUENCE_LENGTH), math.log(8.0 * SEQUENCE_LENGTH)))
    spike_position = jax.random.randint(spike_random_key, (3,), 0, SEQUENCE_LENGTH).astype(jnp.float32)
    spike_factor = jnp.prod(jnp.where(position_index[:, :, None] >= spike_position[None, None, :], 0.7, 1.0), axis=-1)
    slow_mask = kind_draw >= 5
    chan_scale = jnp.exp(jax.random.uniform(scale_random_key, (D, 1), jnp.float32, math.log(0.5), math.log(2.0)))
    decay_length = jnp.where(slow_mask, slow_decay, fast_decay)
    decay_profile = jnp.exp(-position_index / decay_length) * spike_factor
    norm_factor = jnp.sqrt(2.0 / jnp.minimum(decay_length, float(SEQUENCE_LENGTH)))
    return noise_vals * decay_profile * norm_factor * chan_scale


def shard_levels(own_key, extent, pieces, least, top_value):
    gain, own = 1.0, jax.random.fold_in(own_key, 6)
    for axis_at, parts in pieces:
        steps = jnp.exp(jax.random.uniform(jax.random.fold_in(own, axis_at), (parts,), jnp.float32, least / len(pieces), top_value / len(pieces)))
        gain = gain * jnp.repeat(steps, extent[axis_at] // parts).reshape([-1 if axis == axis_at else 1 for axis in range(len(extent))])
    return gain


def bell_draw(own_key, shape, spread, reach, cuts=(), held_as=jnp.bfloat16):
    values = spread * jax.random.normal(own_key, shape, jnp.float32)
    if cuts:
        values = values * shard_levels(own_key, shape, cuts, -0.22, 0.18)
    return jnp.clip(values, -reach, reach).astype(held_as)


def setup_inputs(seed: int = 0) -> dict:
    arg_keys = jax.random.split(jax.random.key(seed), 7)
    query_gate = bell_draw(arg_keys[0], (D, SEQUENCE_LENGTH), 1.0, 6.0, ((1, 128),))
    key_proj = bell_draw(arg_keys[1], (D, SEQUENCE_LENGTH), 1.0, 6.0, ((1, 128),))
    value_proj = bell_draw(arg_keys[2], (D, SEQUENCE_LENGTH), 1.0, 6.0, ((1, 128),))
    out_grad = bell_draw(arg_keys[3], (D, SEQUENCE_LENGTH), 1.0, 6.0, ((1, 128),))
    filters = draw_filters(jax.random.fold_in(arg_keys[6], 71), 0)
    skip_bias = bell_draw(arg_keys[5], (D,), 1.0, 4.0, ((0, 128),), jnp.float32)
    return dict(query_gate=query_gate, key_proj=key_proj, value_proj=value_proj, out_grad=out_grad, filters=filters, skip_bias=skip_bias)


def channel_block(inputs):
    mixed_blk, filter_blk, query_blk, grad_blk, key_blk, value_blk, bias_blk = inputs
    total = 2 * SEQUENCE_LENGTH
    mixed_wide = mixed_blk.astype(jnp.float32)
    mixed_spec = jnp.fft.rfft(mixed_wide, n=total, axis=-1)
    filter_spec = jnp.fft.rfft(filter_blk, n=total, axis=-1)
    conv_rows = jnp.fft.irfft(mixed_spec * filter_spec, n=total, axis=-1)[:, :SEQUENCE_LENGTH]
    bias_col = bias_blk[:, None]
    convolved = (conv_rows + bias_col * mixed_wide).astype(jnp.bfloat16)
    conv_wide = convolved.astype(jnp.float32)
    query_wide = query_blk.astype(jnp.float32)
    grad_wide = grad_blk.astype(jnp.float32)
    output = (query_wide * conv_wide).astype(jnp.bfloat16)
    query_grad = (grad_wide * conv_wide).astype(jnp.bfloat16)
    gated = (grad_wide * query_wide).astype(jnp.bfloat16)
    gated_wide = gated.astype(jnp.float32)
    gated_spec = jnp.fft.rfft(gated_wide, n=total, axis=-1)
    back_rows = jnp.fft.irfft(gated_spec * jnp.conj(filter_spec), n=total, axis=-1)[:, :SEQUENCE_LENGTH]
    mixed_grad = (back_rows + bias_col * gated_wide).astype(jnp.bfloat16)
    grad_wide_mix = mixed_grad.astype(jnp.float32)
    key_grad = (grad_wide_mix * value_blk.astype(jnp.float32)).astype(jnp.bfloat16)
    value_grad = (grad_wide_mix * key_blk.astype(jnp.float32)).astype(jnp.bfloat16)
    grad_scale = 1.0 / math.sqrt(SEQUENCE_LENGTH)
    filter_grad = jnp.fft.irfft(gated_spec * jnp.conj(mixed_spec), n=total, axis=-1)[:, :SEQUENCE_LENGTH] * grad_scale
    bias_grad = lax.optimization_barrier(jnp.sum(gated_wide * mixed_wide, axis=1)) * grad_scale
    return (output, query_grad, key_grad, value_grad, filter_grad, bias_grad)

def reference(query_gate, key_proj, value_proj, out_grad, filters, skip_bias):
    mixed = (key_proj.astype(jnp.float32) * value_proj.astype(jnp.float32)).astype(jnp.bfloat16)
    groups = D // 128

    def split_rows(array):
        return array.reshape(groups, 128, SEQUENCE_LENGTH)
    stacked = (split_rows(mixed), split_rows(filters), split_rows(query_gate), split_rows(out_grad), split_rows(key_proj), split_rows(value_proj), skip_bias.reshape(groups, 128))
    output, query_grad, key_grad, value_grad, filter_grad, bias_grad = lax.map(channel_block, stacked)
    return (output.reshape(D, SEQUENCE_LENGTH), query_grad.reshape(D, SEQUENCE_LENGTH), key_grad.reshape(D, SEQUENCE_LENGTH), value_grad.reshape(D, SEQUENCE_LENGTH), filter_grad.reshape(D, SEQUENCE_LENGTH), bias_grad.reshape(D))
```

```python
import math

import jax
import jax.numpy as jnp
from jax import lax
from jax.experimental import pallas as pl
from jax.experimental.pallas import tpu as pltpu
from jax.sharding import PartitionSpec as P

PRECISE = lax.Precision.HIGHEST


def dft_tables(length):
    padded_len = 2 * length
    fine_len = min(128, length)
    coarse_len = padded_len // fine_len
    coarse_steps = jnp.arange(coarse_len, dtype=jnp.int32)
    coarse_half = jnp.arange(coarse_len // 2, dtype=jnp.int32)
    fine_steps = jnp.arange(fine_len, dtype=jnp.int32)
    coarse_angle = (coarse_steps[:, None] * coarse_half[None, :] % coarse_len).astype(
        jnp.float32
    ) * (2.0 * math.pi / coarse_len)
    twist_angle = (coarse_steps[:, None] * fine_steps[None, :] % padded_len).astype(jnp.float32) * (
        2.0 * math.pi / padded_len
    )
    fine_angle = (fine_steps[:, None] * fine_steps[None, :] % fine_len).astype(jnp.float32) * (
        2.0 * math.pi / fine_len
    )
    return (
        jnp.cos(coarse_angle),
        jnp.sin(coarse_angle),
        jnp.cos(twist_angle),
        jnp.sin(twist_angle),
        jnp.cos(fine_angle),
        jnp.sin(fine_angle),
    )


def forward_transform(signal, tables):
    cos_coarse, sin_coarse, cos_twist, sin_twist, cos_fine, sin_fine = tables
    channels, length = signal.shape
    fine_len = cos_fine.shape[0]
    blocks = signal.reshape(channels, length // fine_len, fine_len)
    first_real = jnp.einsum("ap,cpr->car", cos_coarse, blocks, precision=PRECISE)
    first_imag = -jnp.einsum("ap,cpr->car", sin_coarse, blocks, precision=PRECISE)
    turned_real = (first_real * cos_twist + first_imag * sin_twist).reshape(-1, fine_len)
    turned_imag = (first_imag * cos_twist - first_real * sin_twist).reshape(-1, fine_len)
    spec_real = jnp.dot(turned_real, cos_fine, precision=PRECISE) + jnp.dot(
        turned_imag, sin_fine, precision=PRECISE
    )
    spec_imag = jnp.dot(turned_imag, cos_fine, precision=PRECISE) - jnp.dot(
        turned_real, sin_fine, precision=PRECISE
    )
    return (spec_real, spec_imag)


def inverse_transform(spec_real, spec_imag, tables, channels):
    cos_coarse, sin_coarse, cos_twist, sin_twist, cos_fine, sin_fine = tables
    fine_len = cos_fine.shape[0]
    coarse_len = cos_coarse.shape[0]
    middle_real = jnp.dot(spec_real, cos_fine, precision=PRECISE) - jnp.dot(
        spec_imag, sin_fine, precision=PRECISE
    )
    middle_imag = jnp.dot(spec_imag, cos_fine, precision=PRECISE) + jnp.dot(
        spec_real, sin_fine, precision=PRECISE
    )
    middle_real = middle_real.reshape(channels, coarse_len, fine_len)
    middle_imag = middle_imag.reshape(channels, coarse_len, fine_len)
    turned_real = middle_real * cos_twist - middle_imag * sin_twist
    turned_imag = middle_imag * cos_twist + middle_real * sin_twist
    result = jnp.einsum("ap,car->cpr", cos_coarse, turned_real, precision=PRECISE) - jnp.einsum(
        "ap,car->cpr", sin_coarse, turned_imag, precision=PRECISE
    )
    return result.reshape(channels, -1) * (1.0 / (coarse_len * fine_len))


def multiply(left_spec, right_spec, conjugate):
    left_real, left_imag = left_spec
    right_real, right_imag = right_spec
    if conjugate:
        return (
            left_real * right_real + left_imag * right_imag,
            left_imag * right_real - left_real * right_imag,
        )
    return (
        left_real * right_real - left_imag * right_imag,
        left_real * right_imag + left_imag * right_real,
    )


AXES = ("outer", "inner")
DEVICES = 128


def my_coords():
    outer = lax.axis_index("outer")
    inner = lax.axis_index("inner")
    return outer // 2, (inner // 8) * 2 + outer % 2, (inner // 2) % 4, inner % 2


def partner_at(step, coords):
    z, y, x, core = coords
    mixed_step = (step * 47) % DEVICES
    px = (x + mixed_step) % 4
    pcore = (core + mixed_step // 4) % 2
    py = (y + mixed_step // 8) % 4
    pz = (z + mixed_step // 32) % 4
    return pz * 2 + py % 2, (py // 2) * 8 + px * 2 + pcore


def exchange_kernel(src, dst, send_sem, recv_sem, own_sem):
    coords = my_coords()
    me = lax.axis_index("outer") * 16 + lax.axis_index("inner")
    barrier = pltpu.get_barrier_semaphore()

    @pl.loop(1, DEVICES)
    def _(step):
        outer, inner = partner_at(step, coords)
        pl.semaphore_signal(
            barrier,
            inc=1,
            device_id={"outer": outer, "inner": inner},
            device_id_type=pl.DeviceIdType.MESH,
        )

    own = pltpu.make_async_copy(src.at[me], dst.at[me], own_sem)
    own.start()
    pl.semaphore_wait(barrier, DEVICES - 1)

    @pl.loop(1, DEVICES)
    def _(step):
        outer, inner = partner_at(step, coords)
        pltpu.make_async_remote_copy(
            src_ref=src.at[outer * 16 + inner],
            dst_ref=dst.at[me],
            send_sem=send_sem,
            recv_sem=recv_sem,
            device_id={"outer": outer, "inner": inner},
            device_id_type=pl.DeviceIdType.MESH,
        ).start()

    own.wait()
    rest = dst.at[pl.ds(0, DEVICES - 1)]
    pltpu.make_async_copy(rest, rest, send_sem).wait()
    pltpu.make_async_copy(rest, rest, recv_sem).wait()


def exchange(array, collective_id):
    return pl.pallas_call(
        exchange_kernel,
        out_shape=jax.ShapeDtypeStruct(array.shape, array.dtype),
        in_specs=[pl.BlockSpec(memory_space=pltpu.HBM)],
        out_specs=pl.BlockSpec(memory_space=pltpu.HBM),
        scratch_shapes=[pltpu.SemaphoreType.DMA] * 3,
        compiler_params=pltpu.CompilerParams(collective_id=collective_id, has_side_effects=True),
        name="exchange",
    )(array)


def on_device(query_gate, key_proj, value_proj, out_grad, filters, skip_bias):
    mixed_seq = (key_proj.astype(jnp.float32) * value_proj.astype(jnp.float32)).astype(jnp.bfloat16)
    query_wide = query_gate.astype(jnp.float32)
    grad_wide = out_grad.astype(jnp.float32)
    gated_seq = (grad_wide * query_wide).astype(jnp.bfloat16)
    packed = jnp.concatenate(
        [
            mixed_seq.reshape(DEVICES, 32, 128),
            gated_seq.reshape(DEVICES, 32, 128),
            filters.astype(jnp.bfloat16).reshape(DEVICES, 32, 128),
        ],
        axis=1,
    )
    arrived = exchange(packed, 0)
    mixed_rows, gated_rows, filter_rows = (
        arrived[:, 32 * k : 32 * k + 32].transpose(1, 0, 2).reshape(32, -1) for k in range(3)
    )
    filter_rows = filter_rows.astype(jnp.float32)
    channels, length = mixed_rows.shape
    tables = dft_tables(length)
    filter_spec = forward_transform(filter_rows, tables)
    mixed_wide = mixed_rows.astype(jnp.float32)
    mixed_spec = forward_transform(mixed_wide, tables)
    conv_rows = inverse_transform(*multiply(filter_spec, mixed_spec, False), tables, channels)
    bias_col = skip_bias[:, None]
    convolved_rows = (conv_rows + bias_col * mixed_wide).astype(jnp.bfloat16)
    gated_wide = gated_rows.astype(jnp.float32)
    gated_spec = forward_transform(gated_wide, tables)
    back_rows = inverse_transform(*multiply(gated_spec, filter_spec, True), tables, channels)
    grad_mixed_rows = (back_rows + bias_col * gated_wide).astype(jnp.bfloat16)
    grad_scale = 1.0 / math.sqrt(length)
    filter_rows_grad = (
        inverse_transform(*multiply(gated_spec, mixed_spec, True), tables, channels) * grad_scale
    )
    bias_grad = jnp.sum(gated_wide * mixed_wide, axis=1) * grad_scale
    results = jnp.concatenate(
        [
            rows.reshape(32, DEVICES, 128).transpose(1, 0, 2)
            for rows in (convolved_rows, grad_mixed_rows, filter_rows_grad.astype(jnp.bfloat16))
        ],
        axis=1,
    )
    back = exchange(results, 1)
    convolved, mixed_grad, filter_grad = (back[:, 32 * k : 32 * k + 32].reshape(-1, 128) for k in range(3))
    filter_grad = filter_grad.astype(jnp.float32)
    conv_wide = convolved.astype(jnp.float32)
    output = (query_wide * conv_wide).astype(jnp.bfloat16)
    query_grad = (grad_wide * conv_wide).astype(jnp.bfloat16)
    grad_wide_mix = mixed_grad.astype(jnp.float32)
    key_grad = (grad_wide_mix * value_proj.astype(jnp.float32)).astype(jnp.bfloat16)
    value_grad = (grad_wide_mix * key_proj.astype(jnp.float32)).astype(jnp.bfloat16)
    return (output, query_grad, key_grad, value_grad, filter_grad, bias_grad)


def solution(mesh):
    return jax.shard_map(
        on_device,
        mesh=mesh,
        in_specs=(
            P(None, ("outer", "inner")),
            P(None, ("outer", "inner")),
            P(None, ("outer", "inner")),
            P(None, ("outer", "inner")),
            P(None, ("outer", "inner")),
            P(("outer", "inner")),
        ),
        out_specs=(
            P(None, ("outer", "inner")),
            P(None, ("outer", "inner")),
            P(None, ("outer", "inner")),
            P(None, ("outer", "inner")),
            P(None, ("outer", "inner")),
            P(("outer", "inner")),
        ),
        check_vma=False,
    )
```

```python
import math, functools
import numpy as np
import jax, jax.numpy as jnp
from jax import lax
from jax.experimental import pallas as pl
from jax.experimental.pallas import tpu as pltpu
from jax.sharding import PartitionSpec as P
BF=jnp.bfloat16; F32=jnp.float32
PITCH=136

def split_np(a):
    hi=np.asarray(a,np.float32).astype(BF)
    lo=(np.asarray(a,np.float64)-np.asarray(hi,np.float64)).astype(np.float32).astype(BF)
    return hi,lo

def tables():
    n=128
    k=np.arange(n)[:,None]; p=np.arange(n)[None,:]
    ang=2*np.pi*((p*(2*k+1))%512)/512
    coarse=np.concatenate([np.cos(ang),-np.sin(ang)],0)
    hi,lo=split_np(coarse)
    fwd_coarse=np.concatenate([hi,lo],1)
    inv=np.concatenate([np.cos(ang),-np.sin(ang)],0).T
    hi,lo=split_np(inv)
    inv_coarse=np.concatenate([hi,lo],1)
    ang=2*np.pi*((k*p)%n)/n
    C,S=np.cos(ang),np.sin(ang)
    fw=np.block([[C,-S],[S,C]])
    iv=np.block([[C,S],[-S,C]])
    hi,lo=split_np(fw); fwd_fine=np.concatenate([hi,lo],0)
    hi,lo=split_np(iv); inv_fine=np.concatenate([hi,lo],0)
    tw=2*np.pi*(p*(2*k+1))/65536.0
    twist=np.concatenate([np.cos(tw),np.sin(tw)],0).astype(np.float32)
    return fwd_coarse,inv_coarse,fwd_fine,inv_fine,twist

def dot(a,b): return jnp.dot(a,b,preferred_element_type=F32)
def split(x):
    hi=x.astype(BF); lo=(x-hi.astype(F32)).astype(BF)
    return hi,lo

def spread(recv, work):
    def body(b,_):
        for u in range(4):
            p=b*4+u
            x=recv[p].astype(F32)
            for j in range(6):
                work[pl.ds(8*j*PITCH+p,8,stride=PITCH),:]=x[8*j:8*j+8]
        return 0
    lax.fori_loop(0,32,body,0)

def gather(work, out):
    def body(b,_):
        for u in range(4):
            p=b*4+u
            x=jnp.concatenate([work[pl.ds(8*j*PITCH+p,8,stride=PITCH),:] for j in range(6)],0)
            out[p]=x.astype(BF)
        return 0
    lax.fori_loop(0,32,body,0)

def transforms(pair, work, bias, bias_out, tabs, zs, fs, chunk):
    fwd_coarse,inv_coarse,fwd_fine,inv_fine,twist=tabs
    tc=twist[:128]; ts=twist[128:]
    rows=lambda s,h: (s*16+2*pair+h)*PITCH
    get=lambda s,h: work[pl.ds(pl.multiple_of(rows(s,h),8),128),:]
    for s in range(3):
        x=jnp.concatenate([get(s,0),get(s,1)],1).astype(BF)
        y=dot(fwd_coarse[...],jnp.concatenate([x,x],0))
        for h in range(2):
            yr=y[:128,128*h:128*h+128]; yi=y[128:,128*h:128*h+128]
            zr=yr*tc+yi*ts; zi=yi*tc-yr*ts
            r0=(2*s+h)*128
            for q,z in enumerate((zr,zi)):
                hi,lo=split(z)
                zs[r0:r0+128,128*q:128*q+128]=hi
                zs[r0:r0+128,256+128*q:384+128*q]=lo
    def fine(w):
        zh=zs[:,:256]; zl=zs[:,256:]
        return dot(zh,w[:256])+dot(zh,w[256:])+dot(zl,w[:256])
    fs[...]=fine(fwd_fine)
    for h in range(2):
        part=lambda s,q: fs[(2*s+h)*128:(2*s+h)*128+128,128*q:128*q+128]
        mr,mi,gr,gi,fr,fi=part(0,0),part(0,1),part(1,0),part(1,1),part(2,0),part(2,1)
        prods=((mr*fr-mi*fi,mr*fi+mi*fr),(gr*fr+gi*fi,gi*fr-gr*fi),(gr*mr+gi*mi,gi*mr-gr*mi))
        for s in range(3):
            r0=(2*s+h)*128
            for q in range(2):
                hi,lo=split(prods[s][q])
                zs[r0:r0+128,128*q:128*q+128]=hi
                zs[r0:r0+128,256+128*q:384+128*q]=lo
    fs[...]=fine(inv_fine)
    ys=[]
    for s in range(3):
        cols_h=[];cols_l=[]
        for h in range(2):
            r0=(2*s+h)*128
            ir=fs[r0:r0+128,:128]; ii=fs[r0:r0+128,128:]
            zr=ir*tc-ii*ts; zi=ii*tc+ir*ts
            rh,rl=split(zr); ih,il=split(zi)
            cols_h.append(jnp.concatenate([rh,ih],0)); cols_l.append(jnp.concatenate([rl,il],0))
        zh=jnp.concatenate(cols_h,1); zl=jnp.concatenate(cols_l,1)
        dh=inv_coarse[:,:256]; dl=inv_coarse[:,256:]
        ys.append(dot(dh,zh)+dot(dl,zh)+dot(dh,zl))
    inv_n=1.0/16384.0
    scale=(inv_n,inv_n,inv_n/128.0)
    for h in range(2):
        ch=chunk*16+2*pair+h
        b=bias[ch]
        m=get(0,h); g=get(1,h)
        bias_out[pl.ds(ch,1),:]=jnp.sum(m*g,axis=0,keepdims=True)*(1.0/128.0)
        vals=[ys[s][:,128*h:128*h+128]*scale[s] for s in range(3)]
        vals[0]=vals[0]+b*m
        vals[1]=vals[1]+b*g
        for s in range(3):
            work[pl.ds(pl.multiple_of(rows(s,h),8),128),:]=vals[s]


AXES = ("outer", "inner")
DEVICES = 128


def my_coords():
    outer = lax.axis_index("outer")
    inner = lax.axis_index("inner")
    return outer // 2, (inner // 8) * 2 + outer % 2, (inner // 2) % 4, inner % 2


def partner_at(step, coords):
    z, y, x, core = coords
    mixed_step = (step * 47) % DEVICES
    px = (x + mixed_step) % 4
    pcore = (core + mixed_step // 4) % 2
    py = (y + mixed_step // 8) % 4
    pz = (z + mixed_step // 32) % 4
    return pz * 2 + py % 2, (py // 2) * 8 + px * 2 + pcore


def send_all(src, dst, send_sem, recv_sem, coords, me):
    @pl.loop(1, DEVICES)
    def _(step):
        outer, inner = partner_at(step, coords)
        pltpu.make_async_remote_copy(
            src_ref=src.at[outer * 16 + inner],
            dst_ref=dst.at[me],
            send_sem=send_sem,
            recv_sem=recv_sem,
            device_id={"outer": outer, "inner": inner},
            device_id_type=pl.DeviceIdType.MESH,
        ).start()


def wait_all(buf, sem):
    rest = buf.at[pl.ds(0, DEVICES - 1)]
    pltpu.make_async_copy(rest, rest, sem).wait()


def hyena_kernel(
    bias, src, fwd_coarse, inv_coarse, fwd_fine, inv_fine, twist,
    out, bias_out,
    recv, back, work, zs, fs,
    send_in, recv_in, send_out, recv_out, own_in, own_out,
):
    coords = my_coords()
    me = lax.axis_index("outer") * 16 + lax.axis_index("inner")
    barrier = pltpu.get_barrier_semaphore()

    @pl.loop(1, DEVICES)
    def _(step):
        outer, inner = partner_at(step, coords)
        pl.semaphore_signal(
            barrier,
            inc=1,
            device_id={"outer": outer, "inner": inner},
            device_id_type=pl.DeviceIdType.MESH,
        )

    own = [
        pltpu.make_async_copy(src.at[half, me], recv.at[half, me], own_in.at[half])
        for half in range(2)
    ]
    for copy in own:
        copy.start()
    pl.semaphore_wait(barrier, DEVICES - 1)
    for half in range(2):
        send_all(src.at[half], recv.at[half], send_in.at[half], recv_in.at[half], coords, me)
    tabs = (fwd_coarse, inv_coarse, fwd_fine, inv_fine, twist)
    own_back = []
    for half in range(2):
        own[half].wait()
        wait_all(recv.at[half], recv_in.at[half])
        spread(recv.at[half], work)

        @pl.loop(0, 8)
        def _(pair):
            transforms(pair, work, bias, bias_out, tabs, zs, fs, half)

        gather(work, back.at[half])
        send_all(back.at[half], out.at[half], send_out.at[half], recv_out.at[half], coords, me)
        own_back.append(pltpu.make_async_copy(back.at[half, me], out.at[half, me], own_out.at[half]))
        own_back[half].start()
    for half in range(2):
        own_back[half].wait()
        wait_all(src.at[half], send_in.at[half])
        wait_all(back.at[half], send_out.at[half])
        wait_all(out.at[half], recv_out.at[half])


def hyena_call(bias, packed):
    vmem = pl.BlockSpec(memory_space=pltpu.VMEM)
    hbm = pl.BlockSpec(memory_space=pltpu.HBM)
    return pl.pallas_call(
        hyena_kernel,
        out_shape=(
            jax.ShapeDtypeStruct((2, DEVICES, 48, 128), BF),
            jax.ShapeDtypeStruct((32, 128), F32),
        ),
        in_specs=[pl.BlockSpec(memory_space=pltpu.SMEM), hbm] + [vmem] * 5,
        out_specs=(hbm, vmem),
        scratch_shapes=[
            pltpu.VMEM((2, DEVICES, 48, 128), BF),
            pltpu.VMEM((2, DEVICES, 48, 128), BF),
            pltpu.VMEM((48 * PITCH, 128), F32),
            pltpu.VMEM((768, 512), BF),
            pltpu.VMEM((768, 256), F32),
        ]
        + [pltpu.SemaphoreType.DMA((2,))] * 6,
        compiler_params=pltpu.CompilerParams(
            collective_id=0, has_side_effects=True, vmem_limit_bytes=40 * 2**20
        ),
        name="hyena",
    )(bias, packed, *[jnp.asarray(t) for t in tables()])


def on_device(query_gate, key_proj, value_proj, out_grad, filters, skip_bias):
    key_wide = key_proj.astype(F32)
    value_wide = value_proj.astype(F32)
    query_wide = query_gate.astype(F32)
    grad_wide = out_grad.astype(F32)
    mixed = (key_wide * value_wide).astype(BF)
    gated = (grad_wide * query_wide).astype(BF)

    def halves(array):
        return array.reshape(DEVICES, 2, 16, 128)

    packed = jnp.concatenate(
        [halves(mixed), halves(gated), halves(filters.astype(BF))], axis=2
    ).transpose(1, 0, 2, 3)
    back, bias_rows = hyena_call(skip_bias, packed)

    def result(k):
        return back[:, :, 16 * k : 16 * k + 16].transpose(1, 0, 2, 3).reshape(-1, 128).astype(F32)

    convolved, mixed_grad, filter_grad = (result(k) for k in range(3))
    return (
        (query_wide * convolved).astype(BF),
        (grad_wide * convolved).astype(BF),
        (mixed_grad * value_wide).astype(BF),
        (mixed_grad * key_wide).astype(BF),
        filter_grad,
        jnp.sum(bias_rows, axis=1),
    )


def solution(mesh):
    wide = P(None, AXES)
    return jax.shard_map(
        on_device,
        mesh=mesh,
        in_specs=(wide, wide, wide, wide, wide, P(AXES)),
        out_specs=(wide, wide, wide, wide, wide, P(AXES)),
        check_vma=False,
    )
```

```python
import math, functools
import numpy as np
import jax, jax.numpy as jnp
from jax import lax
from jax.experimental import pallas as pl
from jax.experimental.pallas import tpu as pltpu
from jax.sharding import PartitionSpec as P
BF=jnp.bfloat16; F32=jnp.float32
PITCH=136

def split_np(a):
    hi=np.asarray(a,np.float32).astype(BF)
    lo=(np.asarray(a,np.float64)-np.asarray(hi,np.float64)).astype(np.float32).astype(BF)
    return hi,lo

def tables():
    n=128
    k=np.arange(n)[:,None]; p=np.arange(n)[None,:]
    ang=2*np.pi*((p*(2*k+1))%512)/512
    coarse=np.concatenate([np.cos(ang),-np.sin(ang)],0)
    hi,lo=split_np(coarse)
    fwd_coarse=np.concatenate([hi,lo],1)
    inv=np.concatenate([np.cos(ang),-np.sin(ang)],0).T
    hi,lo=split_np(inv)
    inv_coarse=np.concatenate([hi,lo],1)
    ang=2*np.pi*((k*p)%n)/n
    C,S=np.cos(ang),np.sin(ang)
    fw=np.block([[C,-S],[S,C]])
    iv=np.block([[C,S],[-S,C]])
    hi,lo=split_np(fw); fwd_fine=np.concatenate([hi,lo],0)
    hi,lo=split_np(iv); inv_fine=np.concatenate([hi,lo],0)
    tw=2*np.pi*(p*(2*k+1))/65536.0
    twist=np.concatenate([np.cos(tw),np.sin(tw)],0).astype(np.float32)
    return fwd_coarse,inv_coarse,fwd_fine,inv_fine,twist

def dot(a,b): return jnp.dot(a,b,preferred_element_type=F32)
def split(x):
    hi=x.astype(BF); lo=(x-hi.astype(F32)).astype(BF)
    return hi,lo

def spread(recv, work):
    def body(b,_):
        for u in range(4):
            p=b*4+u
            x=recv[p].astype(F32)
            for j in range(6):
                work[pl.ds(8*j*PITCH+p,8,stride=PITCH),:]=x[8*j:8*j+8]
        return 0
    lax.fori_loop(0,32,body,0)

def gather(work, out):
    def body(b,_):
        for u in range(4):
            p=b*4+u
            x=jnp.concatenate([work[pl.ds(8*j*PITCH+p,8,stride=PITCH),:] for j in range(6)],0)
            out[p]=x.astype(BF)
        return 0
    lax.fori_loop(0,32,body,0)

def transforms(pair, work, bias, bias_out, tabs, zs, fs, chunk):
    fwd_coarse,inv_coarse,fwd_fine,inv_fine,twist=tabs
    tc=twist[:128]; ts=twist[128:]
    rows=lambda s,h: (s*16+2*pair+h)*PITCH
    get=lambda s,h: work[pl.ds(pl.multiple_of(rows(s,h),8),128),:]
    for s in range(3):
        x=jnp.concatenate([get(s,0),get(s,1)],1).astype(BF)
        y=dot(fwd_coarse[...],jnp.concatenate([x,x],0))
        for h in range(2):
            yr=y[:128,128*h:128*h+128]; yi=y[128:,128*h:128*h+128]
            zr=yr*tc+yi*ts; zi=yi*tc-yr*ts
            r0=(2*s+h)*128
            for q,z in enumerate((zr,zi)):
                hi,lo=split(z)
                zs[r0:r0+128,128*q:128*q+128]=hi
                zs[r0:r0+128,256+128*q:384+128*q]=lo
    def fine(w):
        zh=zs[:,:256]; zl=zs[:,256:]
        return dot(zh,w[:256])+dot(zh,w[256:])+dot(zl,w[:256])
    fs[...]=fine(fwd_fine)
    for h in range(2):
        part=lambda s,q: fs[(2*s+h)*128:(2*s+h)*128+128,128*q:128*q+128]
        mr,mi,gr,gi,fr,fi=part(0,0),part(0,1),part(1,0),part(1,1),part(2,0),part(2,1)
        prods=((mr*fr-mi*fi,mr*fi+mi*fr),(gr*fr+gi*fi,gi*fr-gr*fi),(gr*mr+gi*mi,gi*mr-gr*mi))
        for s in range(3):
            r0=(2*s+h)*128
            for q in range(2):
                hi,lo=split(prods[s][q])
                zs[r0:r0+128,128*q:128*q+128]=hi
                zs[r0:r0+128,256+128*q:384+128*q]=lo
    fs[...]=fine(inv_fine)
    ys=[]
    for s in range(3):
        cols_h=[];cols_l=[]
        for h in range(2):
            r0=(2*s+h)*128
            ir=fs[r0:r0+128,:128]; ii=fs[r0:r0+128,128:]
            zr=ir*tc-ii*ts; zi=ii*tc+ir*ts
            rh,rl=split(zr); ih,il=split(zi)
            cols_h.append(jnp.concatenate([rh,ih],0)); cols_l.append(jnp.concatenate([rl,il],0))
        zh=jnp.concatenate(cols_h,1); zl=jnp.concatenate(cols_l,1)
        dh=inv_coarse[:,:256]; dl=inv_coarse[:,256:]
        ys.append(dot(dh,zh)+dot(dl,zh)+dot(dh,zl))
    inv_n=1.0/16384.0
    scale=(inv_n,inv_n,inv_n/128.0)
    for h in range(2):
        ch=chunk*16+2*pair+h
        b=bias[0, ch]
        m=get(0,h); g=get(1,h)
        bias_out[pl.ds(ch,1),:]=jnp.sum(m*g,axis=0,keepdims=True)*(1.0/128.0)
        vals=[ys[s][:,128*h:128*h+128]*scale[s] for s in range(3)]
        vals[0]=vals[0]+b*m
        vals[1]=vals[1]+b*g
        for s in range(3):
            work[pl.ds(pl.multiple_of(rows(s,h),8),128),:]=vals[s]


AXES = ("outer", "inner")
DEVICES = 128
BLOCK = 16


def partners():
    outer = lax.axis_index("outer")
    inner = lax.axis_index("inner")
    z, y, x, core = outer // 2, (inner // 8) * 2 + outer % 2, (inner // 2) % 4, inner % 2
    xs = [(x + k) % 4 for k in range(4)]
    ys = [(y + k) % 4 for k in range(4)]
    zs = [(z + k) % 4 for k in range(4)]
    cores = [(core + k) % 2 for k in range(2)]
    found = []
    for step in range(1, DEVICES):
        mixed_step = (step * 47) % DEVICES
        px, pcore = xs[mixed_step % 4], cores[mixed_step // 4 % 2]
        py, pz = ys[mixed_step // 8 % 4], zs[mixed_step // 32]
        found.append((pz * 2 + py % 2, (py // 2) * 8 + px * 2 + pcore))
    return found


def send_all(src, dst, send_sem, recv_sem, me):
    for outer, inner in partners():
        pltpu.make_async_remote_copy(
            src_ref=src.at[outer * 16 + inner],
            dst_ref=dst.at[me],
            send_sem=send_sem,
            recv_sem=recv_sem,
            device_id={"outer": outer, "inner": inner},
            device_id_type=pl.DeviceIdType.MESH,
        ).start()


def wait_all(buf, sem):
    rest = buf.at[pl.ds(0, DEVICES - 1)]
    pltpu.make_async_copy(rest, rest, sem).wait()


def gate(half, key, value, query, grad, filt, packed):
    @pl.loop(0, DEVICES // 8)
    def _(group):
        at = (pl.ds(pl.multiple_of(group * 8, 8), 8), pl.ds(16 * half, 16))
        put = packed.at[half, at[0]]
        put[:, :16] = (key[at].astype(F32) * value[at].astype(F32)).astype(BF)
        put[:, 16:32] = (grad[at].astype(F32) * query[at].astype(F32)).astype(BF)
        put[:, 32:] = filt[at].astype(BF)


def hyena_kernel(
    key_in, value_in, query_in, grad_in, filt_in, *rest,
):
    tabs_in, rest = rest[:6], rest[6:]
    out, bias_out, key, value, query, grad = rest[:6]
    tabs, rest = rest[6:12], rest[12:]
    filt, packed, recv, back, work, zs, fs, send_in, recv_in, send_out, recv_out, own_out, load = rest
    bias, tabs = tabs[0], tabs[1:]
    me = lax.axis_index("outer") * 16 + lax.axis_index("inner")
    loads = [
        pltpu.make_async_copy(src, dst, load.at[k])
        for k, (src, dst) in enumerate(
            (
                (key_in, key), (value_in, value), (grad_in, grad), (query_in, query), (filt_in, filt),
                *zip(tabs_in, (bias, *tabs)),
            )
        )
    ]
    for copy in loads:
        copy.start()
    barrier = pltpu.get_barrier_semaphore()
    with jax.named_scope("bar_signal"):
        for outer, inner in partners():
            pl.semaphore_signal(
                barrier,
                inc=1,
                device_id={"outer": outer, "inner": inner},
                device_id_type=pl.DeviceIdType.MESH,
            )
    with jax.named_scope("loads"):
        for copy in loads[:5]:
            copy.wait()
    with jax.named_scope("gate0"):
        gate(0, key, value, query, grad, filt, packed)
    with jax.named_scope("bar_wait"):
        pl.semaphore_wait(barrier, DEVICES - 1)
    send_all(packed.at[0], recv.at[0], send_in.at[0], recv_in.at[0], me)
    recv[0, me] = packed[0, me]
    with jax.named_scope("gate1"):
        gate(1, key, value, query, grad, filt, packed)
    recv[1, me] = packed[1, me]
    with jax.named_scope("sent_in0"):
        wait_all(packed.at[0], send_in.at[0])
    send_all(packed.at[1], recv.at[1], send_in.at[1], recv_in.at[1], me)
    for copy in loads[5:]:
        copy.wait()
    own_back = []
    for half in range(2):
        with jax.named_scope(f"wait_in{half}"):
            wait_all(recv.at[half], recv_in.at[half])
        spread(recv.at[half], work)

        with jax.named_scope(f"transforms{half}"):

            @pl.loop(0, 8)
            def _(pair):
                transforms(pair, work, bias, bias_out, tabs, zs, fs, half)

        gather(work, back.at[half])
        with jax.named_scope(f"send_out{half}"):
            send_all(back.at[half], out.at[half], send_out.at[half], recv_out.at[half], me)
        own_back.append(pltpu.make_async_copy(back.at[half, me], out.at[half, me], own_out.at[half]))
        own_back[half].start()
    wait_all(packed.at[1], send_in.at[1])
    for half in range(2):
        own_back[half].wait()
        wait_all(back.at[half], send_out.at[half])
        with jax.named_scope(f"wait_out{half}"):
            wait_all(out.at[half], recv_out.at[half])


def hyena_call(bias, key, value, query, grad, filt):
    consts = [jnp.asarray(t) for t in tables()]
    vmem = pl.BlockSpec(memory_space=pltpu.VMEM)
    hbm = pl.BlockSpec(memory_space=pltpu.HBM)
    rows = jax.ShapeDtypeStruct((DEVICES, 32, 128), BF)
    return pl.pallas_call(
        hyena_kernel,
        out_shape=(
            jax.ShapeDtypeStruct((2, DEVICES, 48, 128), BF),
            jax.ShapeDtypeStruct((32, 128), F32),
            rows, rows, rows, rows,
        ),
        in_specs=[hbm] * 11,
        out_specs=(hbm,) + (vmem,) * 5,
        scratch_shapes=[pltpu.SMEM((1, 32), F32)]
        + [pltpu.VMEM(t.shape, t.dtype) for t in consts]
        + [
            pltpu.VMEM((DEVICES, 32, 128), F32),
            pltpu.VMEM((2, DEVICES, 48, 128), BF),
            pltpu.VMEM((2, DEVICES, 48, 128), BF),
            pltpu.VMEM((2, DEVICES, 48, 128), BF),
            pltpu.VMEM((48 * PITCH, 128), F32),
            pltpu.VMEM((768, 512), BF),
            pltpu.VMEM((768, 256), F32),
        ]
        + [pltpu.SemaphoreType.DMA((2,))] * 5
        + [pltpu.SemaphoreType.DMA((11,))],
        compiler_params=pltpu.CompilerParams(
            collective_id=0, has_side_effects=True, vmem_limit_bytes=40 * 2**20
        ),
        name="hyena",
    )(
        *[
            pltpu.with_memory_space_constraint(t, pltpu.HBM)
            for t in (key, value, query, grad, filt, bias.reshape(1, 32), *consts)
        ]
    )


def finish_kernel(back, bias_rows, key, value, query, grad, output, query_grad, key_grad, value_grad, filter_grad, bias_grad):
    step = pl.program_id(0)
    at = pl.ds(pl.multiple_of(step * BLOCK, BLOCK), BLOCK)
    for half in range(2):
        rows = slice(16 * half, 16 * half + 16)
        convolved = back[half, at, :16].astype(F32)
        mixed_grad = back[half, at, 16:32].astype(F32)
        output[:, rows] = (query[at, rows].astype(F32) * convolved).astype(BF)
        query_grad[:, rows] = (grad[at, rows].astype(F32) * convolved).astype(BF)
        key_grad[:, rows] = (value[at, rows].astype(F32) * mixed_grad).astype(BF)
        value_grad[:, rows] = (key[at, rows].astype(F32) * mixed_grad).astype(BF)
        filter_grad[:, rows] = back[half, at, 32:].astype(F32)

    @pl.when(step == 0)
    def _():
        bias_grad[...] = jnp.sum(bias_rows[...].T, axis=0, keepdims=True)


def finish_call(*args):
    vmem = pl.BlockSpec(memory_space=pltpu.VMEM)
    block = pl.BlockSpec((BLOCK, 32, 128), lambda i: (i, 0, 0))
    rows = jax.ShapeDtypeStruct((DEVICES, 32, 128), BF)
    return pl.pallas_call(
        finish_kernel,
        grid=(DEVICES // BLOCK,),
        out_shape=(rows, rows, rows, rows, jax.ShapeDtypeStruct((DEVICES, 32, 128), F32), jax.ShapeDtypeStruct((1, 32), F32)),
        in_specs=[vmem] * 6,
        out_specs=(block,) * 5 + (pl.BlockSpec((1, 32), lambda i: (0, 0)),),
        compiler_params=pltpu.CompilerParams(vmem_limit_bytes=16 * 2**20),
        name="finish",
    )(*args)


def on_device(query_gate, key_proj, value_proj, out_grad, filters, skip_bias):
    def rows(array):
        return array.reshape(DEVICES, 32, 128)

    back, bias_rows, key, value, query, grad = hyena_call(
        skip_bias, rows(key_proj), rows(value_proj), rows(query_gate), rows(out_grad), rows(filters)
    )
    *grads, bias_grad = finish_call(back, bias_rows, key, value, query, grad)
    return (*[array.reshape(-1, 128) for array in grads], bias_grad.reshape(-1))


def solution(mesh):
    wide = P(None, AXES)
    return jax.shard_map(
        on_device,
        mesh=mesh,
        in_specs=(wide, wide, wide, wide, wide, P(AXES)),
        out_specs=(wide, wide, wide, wide, wide, P(AXES)),
        check_vma=False,
    )
```

```python
import math, functools
import numpy as np
import jax, jax.numpy as jnp
from jax import lax
from jax.experimental import pallas as pl
from jax.experimental.pallas import tpu as pltpu
from jax.sharding import PartitionSpec as P
BF=jnp.bfloat16; F32=jnp.float32
PITCH=136

def split_np(a):
    hi=np.asarray(a,np.float32).astype(BF)
    lo=(np.asarray(a,np.float64)-np.asarray(hi,np.float64)).astype(np.float32).astype(BF)
    return hi,lo

def tables():
    n=128
    k=np.arange(n)[:,None]; p=np.arange(n)[None,:]
    ang=2*np.pi*((p*(2*k+1))%512)/512
    coarse=np.concatenate([np.cos(ang),-np.sin(ang)],0)
    hi,lo=split_np(coarse)
    fwd_coarse=np.concatenate([hi,lo],1)
    inv=np.concatenate([np.cos(ang),-np.sin(ang)],0).T
    hi,lo=split_np(inv)
    inv_coarse=np.concatenate([hi,lo],1)
    ang=2*np.pi*((k*p)%n)/n
    C,S=np.cos(ang),np.sin(ang)
    fw=np.block([[C,-S],[S,C]])
    iv=np.block([[C,S],[-S,C]])
    hi,lo=split_np(fw); fwd_fine=np.concatenate([hi,lo],0)
    hi,lo=split_np(iv); inv_fine=np.concatenate([hi,lo],0)
    tw=2*np.pi*(p*(2*k+1))/65536.0
    twist=np.concatenate([np.cos(tw),np.sin(tw)],0).astype(np.float32)
    return fwd_coarse,inv_coarse,fwd_fine,inv_fine,twist

def dot(a,b): return jnp.dot(a,b,preferred_element_type=F32)
def split(x):
    hi=x.astype(BF); lo=(x-hi.astype(F32)).astype(BF)
    return hi,lo

def spread(recv, work):
    def body(b,_):
        for u in range(4):
            p=b*4+u
            x=recv[p].astype(F32)
            for j in range(6):
                work[pl.ds(8*j*PITCH+p,8,stride=PITCH),:]=x[8*j:8*j+8]
        return 0
    lax.fori_loop(0,32,body,0)

def gather(work, out):
    def body(b,_):
        for u in range(4):
            p=b*4+u
            x=jnp.concatenate([work[pl.ds(8*j*PITCH+p,8,stride=PITCH),:] for j in range(6)],0)
            out[p]=x.astype(BF)
        return 0
    lax.fori_loop(0,32,body,0)

def run_pairs(work, bias, bias_out, tabs, zf, ff, zi, fi, half):
    fwd_coarse, inv_coarse, fwd_fine, inv_fine, twist = tabs
    tc = twist[:128]
    ts = twist[128:]

    def rows(pair, s, h):
        return pl.ds(pl.multiple_of((s * 16 + 2 * pair + h) * PITCH, 8), 128)

    def put(z, r0, q, value):
        hi, lo = split(value)
        z[r0 : r0 + 128, 128 * q : 128 * q + 128] = hi
        z[r0 : r0 + 128, 256 + 128 * q : 384 + 128 * q] = lo

    def fine(z, f, w, r0, r1):
        zh = z[r0:r1, :256]
        f[r0:r1] = dot(zh, w[:256]) + dot(zh, w[256:]) + dot(z[r0:r1, 256:], w[:256])

    def coarse(pair, s):
        x = jnp.concatenate([work[rows(pair, s, 0), :], work[rows(pair, s, 1), :]], 1).astype(BF)
        return dot(fwd_coarse[...], jnp.concatenate([x, x], 0))

    def turn(s, y):
        for h in range(2):
            yr = y[:128, 128 * h : 128 * h + 128]
            yi = y[128:, 128 * h : 128 * h + 128]
            put(zf, (2 * s + h) * 128, 0, yr * tc + yi * ts)
            put(zf, (2 * s + h) * 128, 1, yi * tc - yr * ts)

    def spectra(s):
        fine(zf, ff, fwd_fine, 2 * s * 128, 2 * s * 128 + 256)

    def products(h):
        mr, mi, gr, gi, fr, fi_ = (
            ff[(2 * s + h) * 128 : (2 * s + h) * 128 + 128, 128 * q : 128 * q + 128]
            for s in range(3)
            for q in range(2)
        )
        for s, pairs in enumerate(
            (
                (mr * fr - mi * fi_, mr * fi_ + mi * fr),
                (gr * fr + gi * fi_, gi * fr - gr * fi_),
                (gr * mr + gi * mi, gi * mr - gr * mi),
            )
        ):
            for q in range(2):
                put(zi, (3 * h + s) * 128, q, pairs[q])

    def back_fine(h):
        fine(zi, fi, inv_fine, 3 * h * 128, 3 * h * 128 + 384)

    def back_turn(s):
        his, los = [], []
        for h in range(2):
            r0 = (3 * h + s) * 128
            ir = fi[r0 : r0 + 128, :128]
            ii = fi[r0 : r0 + 128, 128:]
            rh, rl = split(ir * tc - ii * ts)
            ih, il = split(ii * tc + ir * ts)
            his.append(jnp.concatenate([rh, ih], 0))
            los.append(jnp.concatenate([rl, il], 0))
        return jnp.concatenate(his, 1), jnp.concatenate(los, 1)

    def back_coarse(pair, s, z):
        dh = inv_coarse[:, :256]
        y = dot(dh, z[0]) + dot(inv_coarse[:, 256:], z[0]) + dot(dh, z[1])
        for h in range(2):
            value = y[:, 128 * h : 128 * h + 128] * (1.0 / 16384.0 if s < 2 else 1.0 / 2097152.0)
            channel = half * 16 + 2 * pair + h
            if s < 2:
                own = work[rows(pair, s, h), :]
                if s == 0:
                    bias_out[pl.ds(channel, 1), :] = jnp.sum(
                        own * work[rows(pair, 1, h), :], axis=0, keepdims=True
                    ) * (1.0 / 128.0)
                value = value + bias[0, channel] * own
            work[rows(pair, s, h), :] = value

    for s in range(3):
        turn(s, coarse(0, s))
        spectra(s)

    @pl.loop(0, 7)
    def _(pair):
        y0 = coarse(pair + 1, 0)
        products(0)
        y1 = coarse(pair + 1, 1)
        products(1)
        back_fine(0)
        turn(0, y0)
        y2 = coarse(pair + 1, 2)
        back_fine(1)
        turn(1, y1)
        spectra(0)
        turn(2, y2)
        z0 = back_turn(0)
        spectra(1)
        back_coarse(pair, 0, z0)
        z1 = back_turn(1)
        spectra(2)
        back_coarse(pair, 1, z1)
        back_coarse(pair, 2, back_turn(2))

    for h in range(2):
        products(h)
        back_fine(h)
    for s in range(3):
        back_coarse(7, s, back_turn(s))


AXES = ("outer", "inner")
DEVICES = 128
BLOCK = 16


def partners():
    outer = lax.axis_index("outer")
    inner = lax.axis_index("inner")
    z, y, x, core = outer // 2, (inner // 8) * 2 + outer % 2, (inner // 2) % 4, inner % 2
    xs = [(x + k) % 4 for k in range(4)]
    ys = [(y + k) % 4 for k in range(4)]
    zs = [(z + k) % 4 for k in range(4)]
    cores = [(core + k) % 2 for k in range(2)]
    found = []
    for step in range(1, DEVICES):
        mixed_step = (step * 47) % DEVICES
        px, pcore = xs[mixed_step % 4], cores[mixed_step // 4 % 2]
        py, pz = ys[mixed_step // 8 % 4], zs[mixed_step // 32]
        found.append((pz * 2 + py % 2, (py // 2) * 8 + px * 2 + pcore))
    return found


def send_all(src, dst, send_sem, recv_sem, me):
    for outer, inner in partners():
        pltpu.make_async_remote_copy(
            src_ref=src.at[outer * 16 + inner],
            dst_ref=dst.at[me],
            send_sem=send_sem,
            recv_sem=recv_sem,
            device_id={"outer": outer, "inner": inner},
            device_id_type=pl.DeviceIdType.MESH,
        ).start()


def wait_all(buf, sem):
    rest = buf.at[pl.ds(0, DEVICES - 1)]
    pltpu.make_async_copy(rest, rest, sem).wait()


def gate(half, key, value, query, grad, filt, packed):
    @pl.loop(0, DEVICES // 8)
    def _(group):
        at = (pl.ds(pl.multiple_of(group * 8, 8), 8), pl.ds(16 * half, 16))
        put = packed.at[half, at[0]]
        put[:, :16] = (key[at].astype(F32) * value[at].astype(F32)).astype(BF)
        put[:, 16:32] = (grad[at].astype(F32) * query[at].astype(F32)).astype(BF)
        put[:, 32:] = filt[at].astype(BF)


def hyena_kernel(
    key_in, value_in, query_in, grad_in, filt_in, *rest,
):
    tabs_in, rest = rest[:6], rest[6:]
    out, bias_out, key, value, query, grad = rest[:6]
    tabs, rest = rest[6:12], rest[12:]
    filt, packed, recv, back, work, zf, ff, zi, fi, send_in, recv_in, send_out, recv_out, own_out, load = rest
    bias, tabs = tabs[0], tabs[1:]
    me = lax.axis_index("outer") * 16 + lax.axis_index("inner")
    loads = [
        pltpu.make_async_copy(src, dst, load.at[k])
        for k, (src, dst) in enumerate(
            (
                (key_in, key), (value_in, value), (grad_in, grad), (query_in, query), (filt_in, filt),
                *zip(tabs_in, (bias, *tabs)),
            )
        )
    ]
    for copy in loads:
        copy.start()
    barrier = pltpu.get_barrier_semaphore()
    with jax.named_scope("bar_signal"):
        for outer, inner in partners():
            pl.semaphore_signal(
                barrier,
                inc=1,
                device_id={"outer": outer, "inner": inner},
                device_id_type=pl.DeviceIdType.MESH,
            )
    with jax.named_scope("loads"):
        for copy in loads[:5]:
            copy.wait()
    with jax.named_scope("gate0"):
        gate(0, key, value, query, grad, filt, packed)
    with jax.named_scope("bar_wait"):
        pl.semaphore_wait(barrier, DEVICES - 1)
    send_all(packed.at[0], recv.at[0], send_in.at[0], recv_in.at[0], me)
    recv[0, me] = packed[0, me]
    with jax.named_scope("gate1"):
        gate(1, key, value, query, grad, filt, packed)
    recv[1, me] = packed[1, me]
    with jax.named_scope("sent_in0"):
        wait_all(packed.at[0], send_in.at[0])
    send_all(packed.at[1], recv.at[1], send_in.at[1], recv_in.at[1], me)
    for copy in loads[5:]:
        copy.wait()
    own_back = []
    for half in range(2):
        with jax.named_scope(f"wait_in{half}"):
            wait_all(recv.at[half], recv_in.at[half])
        spread(recv.at[half], work)

        with jax.named_scope(f"transforms{half}"):
            run_pairs(work, bias, bias_out, tabs, zf, ff, zi, fi, half)

        gather(work, back.at[half])
        with jax.named_scope(f"send_out{half}"):
            send_all(back.at[half], out.at[half], send_out.at[half], recv_out.at[half], me)
        own_back.append(pltpu.make_async_copy(back.at[half, me], out.at[half, me], own_out.at[half]))
        own_back[half].start()
    wait_all(packed.at[1], send_in.at[1])
    for half in range(2):
        own_back[half].wait()
        wait_all(back.at[half], send_out.at[half])
        with jax.named_scope(f"wait_out{half}"):
            wait_all(out.at[half], recv_out.at[half])


def hyena_call(bias, key, value, query, grad, filt):
    consts = [jnp.asarray(t) for t in tables()]
    vmem = pl.BlockSpec(memory_space=pltpu.VMEM)
    hbm = pl.BlockSpec(memory_space=pltpu.HBM)
    rows = jax.ShapeDtypeStruct((DEVICES, 32, 128), BF)
    return pl.pallas_call(
        hyena_kernel,
        out_shape=(
            jax.ShapeDtypeStruct((2, DEVICES, 48, 128), BF),
            jax.ShapeDtypeStruct((32, 128), F32),
            rows, rows, rows, rows,
        ),
        in_specs=[hbm] * 11,
        out_specs=(hbm,) + (vmem,) * 5,
        scratch_shapes=[pltpu.SMEM((1, 32), F32)]
        + [pltpu.VMEM(t.shape, t.dtype) for t in consts]
        + [
            pltpu.VMEM((DEVICES, 32, 128), F32),
            pltpu.VMEM((2, DEVICES, 48, 128), BF),
            pltpu.VMEM((2, DEVICES, 48, 128), BF),
            pltpu.VMEM((2, DEVICES, 48, 128), BF),
            pltpu.VMEM((48 * PITCH, 128), F32),
            pltpu.VMEM((768, 512), BF),
            pltpu.VMEM((768, 256), F32),
            pltpu.VMEM((768, 512), BF),
            pltpu.VMEM((768, 256), F32),
        ]
        + [pltpu.SemaphoreType.DMA((2,))] * 5
        + [pltpu.SemaphoreType.DMA((11,))],
        compiler_params=pltpu.CompilerParams(
            collective_id=0, has_side_effects=True, vmem_limit_bytes=40 * 2**20
        ),
        name="hyena",
    )(
        *[
            pltpu.with_memory_space_constraint(t, pltpu.HBM)
            for t in (key, value, query, grad, filt, bias.reshape(1, 32), *consts)
        ]
    )


def finish_kernel(back, bias_rows, key, value, query, grad, output, query_grad, key_grad, value_grad, filter_grad, bias_grad):
    step = pl.program_id(0)
    at = pl.ds(pl.multiple_of(step * BLOCK, BLOCK), BLOCK)
    for half in range(2):
        rows = slice(16 * half, 16 * half + 16)
        convolved = back[half, at, :16].astype(F32)
        mixed_grad = back[half, at, 16:32].astype(F32)
        output[:, rows] = (query[at, rows].astype(F32) * convolved).astype(BF)
        query_grad[:, rows] = (grad[at, rows].astype(F32) * convolved).astype(BF)
        key_grad[:, rows] = (value[at, rows].astype(F32) * mixed_grad).astype(BF)
        value_grad[:, rows] = (key[at, rows].astype(F32) * mixed_grad).astype(BF)
        filter_grad[:, rows] = back[half, at, 32:].astype(F32)

    @pl.when(step == 0)
    def _():
        bias_grad[...] = jnp.sum(bias_rows[...].T, axis=0, keepdims=True)


def finish_call(*args):
    vmem = pl.BlockSpec(memory_space=pltpu.VMEM)
    block = pl.BlockSpec((BLOCK, 32, 128), lambda i: (i, 0, 0))
    rows = jax.ShapeDtypeStruct((DEVICES, 32, 128), BF)
    return pl.pallas_call(
        finish_kernel,
        grid=(DEVICES // BLOCK,),
        out_shape=(rows, rows, rows, rows, jax.ShapeDtypeStruct((DEVICES, 32, 128), F32), jax.ShapeDtypeStruct((1, 32), F32)),
        in_specs=[vmem] * 6,
        out_specs=(block,) * 5 + (pl.BlockSpec((1, 32), lambda i: (0, 0)),),
        compiler_params=pltpu.CompilerParams(vmem_limit_bytes=16 * 2**20),
        name="finish",
    )(*args)


def on_device(query_gate, key_proj, value_proj, out_grad, filters, skip_bias):
    def rows(array):
        return array.reshape(DEVICES, 32, 128)

    back, bias_rows, key, value, query, grad = hyena_call(
        skip_bias, rows(key_proj), rows(value_proj), rows(query_gate), rows(out_grad), rows(filters)
    )
    *grads, bias_grad = finish_call(back, bias_rows, key, value, query, grad)
    return (*[array.reshape(-1, 128) for array in grads], bias_grad.reshape(-1))


def solution(mesh):
    wide = P(None, AXES)
    return jax.shard_map(
        on_device,
        mesh=mesh,
        in_specs=(wide, wide, wide, wide, wide, P(AXES)),
        out_specs=(wide, wide, wide, wide, wide, P(AXES)),
        check_vma=False,
    )
```

```python
import math, functools
import numpy as np
import jax, jax.numpy as jnp
from jax import lax
from jax.experimental import pallas as pl
from jax.experimental.pallas import tpu as pltpu
from jax.sharding import PartitionSpec as P
BF=jnp.bfloat16; F32=jnp.float32
PITCH=136

def split_np(a):
    hi=np.asarray(a,np.float32).astype(BF)
    lo=(np.asarray(a,np.float64)-np.asarray(hi,np.float64)).astype(np.float32).astype(BF)
    return hi,lo

def tables():
    n=128
    k=np.arange(n)[:,None]; p=np.arange(n)[None,:]
    ang=2*np.pi*((p*(2*k+1))%512)/512
    coarse=np.concatenate([np.cos(ang),-np.sin(ang)],0)
    hi,lo=split_np(coarse)
    fwd_coarse=np.concatenate([hi,lo],1)
    inv=np.concatenate([np.cos(ang),-np.sin(ang)],0).T
    hi,lo=split_np(inv)
    inv_coarse=np.concatenate([hi,lo],1)
    ang=2*np.pi*((k*p)%n)/n
    C,S=np.cos(ang),np.sin(ang)
    fw=np.block([[C,-S],[S,C]])
    iv=np.block([[C,S],[-S,C]])
    hi,lo=split_np(fw); fwd_fine=np.concatenate([hi,lo],0)
    hi,lo=split_np(iv); inv_fine=np.concatenate([hi,lo],0)
    tw=2*np.pi*(p*(2*k+1))/65536.0
    twist=np.concatenate([np.cos(tw),np.sin(tw)],0).astype(np.float32)
    return fwd_coarse,inv_coarse,fwd_fine,inv_fine,twist

def dot(a,b): return jnp.dot(a,b,preferred_element_type=F32)
def split(x):
    hi=x.astype(BF); lo=(x-hi.astype(F32)).astype(BF)
    return hi,lo

def spread(recv, work):
    def body(b,_):
        for u in range(4):
            p=b*4+u
            x=recv[p].astype(F32)
            for j in range(6):
                work[pl.ds(8*j*PITCH+p,8,stride=PITCH),:]=x[8*j:8*j+8]
        return 0
    lax.fori_loop(0,32,body,0)

def gather(work, out):
    def body(b,_):
        for u in range(4):
            p=b*4+u
            x=jnp.concatenate([work[pl.ds(8*j*PITCH+p,8,stride=PITCH),:] for j in range(6)],0)
            out[p]=x.astype(BF)
        return 0
    lax.fori_loop(0,32,body,0)

def run_pairs(work, bias, bias_out, tabs, zf, ff, zi, fi, half):
    fwd_coarse, inv_coarse, fwd_fine, inv_fine, twist = tabs
    tc = twist[:128]
    ts = twist[128:]

    def rows(pair, s, h):
        return pl.ds(pl.multiple_of((s * 16 + 2 * pair + h) * PITCH, 8), 128)

    def put(z, r0, q, value):
        hi, lo = split(value)
        z[r0 : r0 + 128, 128 * q : 128 * q + 128] = hi
        z[r0 : r0 + 128, 256 + 128 * q : 384 + 128 * q] = lo

    def fine(z, f, w, r0, r1):
        zh = z[r0:r1, :256]
        f[r0:r1] = dot(zh, w[:256]) + dot(zh, w[256:]) + dot(z[r0:r1, 256:], w[:256])

    def coarse(pair, s):
        x = jnp.concatenate([work[rows(pair, s, 0), :], work[rows(pair, s, 1), :]], 1).astype(BF)
        return dot(fwd_coarse[...], jnp.concatenate([x, x], 0))

    def turn(s, y):
        for h in range(2):
            yr = y[:128, 128 * h : 128 * h + 128]
            yi = y[128:, 128 * h : 128 * h + 128]
            put(zf, (2 * s + h) * 128, 0, yr * tc + yi * ts)
            put(zf, (2 * s + h) * 128, 1, yi * tc - yr * ts)

    def spectra(s):
        fine(zf, ff, fwd_fine, 2 * s * 128, 2 * s * 128 + 256)

    def products(h):
        mr, mi, gr, gi, fr, fi_ = (
            ff[(2 * s + h) * 128 : (2 * s + h) * 128 + 128, 128 * q : 128 * q + 128]
            for s in range(3)
            for q in range(2)
        )
        for s, pairs in enumerate(
            (
                (mr * fr - mi * fi_, mr * fi_ + mi * fr),
                (gr * fr + gi * fi_, gi * fr - gr * fi_),
                (gr * mr + gi * mi, gi * mr - gr * mi),
            )
        ):
            for q in range(2):
                put(zi, (3 * h + s) * 128, q, pairs[q])

    def back_fine(h):
        fine(zi, fi, inv_fine, 3 * h * 128, 3 * h * 128 + 384)

    def back_turn(s):
        his, los = [], []
        for h in range(2):
            r0 = (3 * h + s) * 128
            ir = fi[r0 : r0 + 128, :128]
            ii = fi[r0 : r0 + 128, 128:]
            rh, rl = split(ir * tc - ii * ts)
            ih, il = split(ii * tc + ir * ts)
            his.append(jnp.concatenate([rh, ih], 0))
            los.append(jnp.concatenate([rl, il], 0))
        return jnp.concatenate(his, 1), jnp.concatenate(los, 1)

    def back_coarse(pair, s, z):
        dh = inv_coarse[:, :256]
        y = dot(dh, z[0]) + dot(inv_coarse[:, 256:], z[0]) + dot(dh, z[1])
        for h in range(2):
            value = y[:, 128 * h : 128 * h + 128] * (1.0 / 16384.0 if s < 2 else 1.0 / 2097152.0)
            channel = half * 16 + 2 * pair + h
            if s < 2:
                own = work[rows(pair, s, h), :]
                if s == 0:
                    bias_out[pl.ds(channel, 1), :] = jnp.sum(
                        own * work[rows(pair, 1, h), :], axis=0, keepdims=True
                    ) * (1.0 / 128.0)
                value = value + bias[0, channel] * own
            work[rows(pair, s, h), :] = value

    for s in range(3):
        turn(s, coarse(0, s))
        spectra(s)

    @pl.loop(0, 7)
    def _(pair):
        y0 = coarse(pair + 1, 0)
        products(0)
        y1 = coarse(pair + 1, 1)
        products(1)
        back_fine(0)
        turn(0, y0)
        y2 = coarse(pair + 1, 2)
        back_fine(1)
        turn(1, y1)
        spectra(0)
        turn(2, y2)
        z0 = back_turn(0)
        spectra(1)
        back_coarse(pair, 0, z0)
        z1 = back_turn(1)
        spectra(2)
        back_coarse(pair, 1, z1)
        back_coarse(pair, 2, back_turn(2))

    for h in range(2):
        products(h)
        back_fine(h)
    for s in range(3):
        back_coarse(7, s, back_turn(s))


AXES = ("outer", "inner")
DEVICES = 128
BLOCK = 16
ORDER = (
    85, 1, 84, 96, 52, 8, 92, 25, 77, 7, 83, 6, 82, 32, 116, 24,
    76, 97, 53, 2, 86, 3, 87, 33, 117, 9, 93, 39, 114, 5, 81, 15,
    91, 17, 69, 40, 124, 10, 95, 102, 51, 34, 119, 11, 94, 31, 75, 26,
    79, 121, 44, 65, 21, 120, 45, 38, 115, 105, 60, 57, 108, 104, 61, 41,
    125, 14, 90, 30, 74, 35, 118, 99, 54, 56, 109, 4, 80, 27, 78, 64,
    20, 16, 68, 98, 55, 103, 50, 127, 42, 46, 122, 37, 113, 22, 67, 100,
    48, 23, 66, 88, 12, 47, 123, 62, 106, 36, 112, 72, 29, 110, 59, 19,
    71, 89, 13, 43, 126, 111, 58, 28, 73, 70, 18, 107, 63, 101, 49,
)


def partners():
    outer = lax.axis_index("outer")
    inner = lax.axis_index("inner")
    z, y, x, core = outer // 2, (inner // 8) * 2 + outer % 2, (inner // 2) % 4, inner % 2
    xs = [(x + k) % 4 for k in range(4)]
    ys = [(y + k) % 4 for k in range(4)]
    zs = [(z + k) % 4 for k in range(4)]
    cores = [(core + k) % 2 for k in range(2)]
    found = []
    for code in ORDER:
        px, pcore = xs[code // 2 % 4], cores[code % 2]
        py, pz = ys[code // 8 % 4], zs[code // 32]
        found.append((pz * 2 + py % 2, (py // 2) * 8 + px * 2 + pcore))
    return found


def send_all(src, dst, send_sem, recv_sem, me):
    for outer, inner in partners():
        pltpu.make_async_remote_copy(
            src_ref=src.at[outer * 16 + inner],
            dst_ref=dst.at[me],
            send_sem=send_sem,
            recv_sem=recv_sem,
            device_id={"outer": outer, "inner": inner},
            device_id_type=pl.DeviceIdType.MESH,
        ).start()


def wait_all(buf, sem):
    rest = buf.at[pl.ds(0, DEVICES - 1)]
    pltpu.make_async_copy(rest, rest, sem).wait()


def gate(half, key, value, query, grad, filt, packed):
    @pl.loop(0, DEVICES // 8)
    def _(group):
        at = (pl.ds(pl.multiple_of(group * 8, 8), 8), pl.ds(16 * half, 16))
        put = packed.at[half, at[0]]
        put[:, :16] = (key[at].astype(F32) * value[at].astype(F32)).astype(BF)
        put[:, 16:32] = (grad[at].astype(F32) * query[at].astype(F32)).astype(BF)
        put[:, 32:] = filt[at].astype(BF)


def hyena_kernel(
    key_in, value_in, query_in, grad_in, filt_in, *rest,
):
    tabs_in, rest = rest[:6], rest[6:]
    out, bias_out, key, value, query, grad, filt = rest[:7]
    tabs, rest = rest[7:13], rest[13:]
    early, packed, recv, back, work, zf, ff, zi, fi, send_in, recv_in, send_out, recv_out, own_out, load = rest
    bias, tabs = tabs[0], tabs[1:]
    me = lax.axis_index("outer") * 16 + lax.axis_index("inner")
    fields = (
        (key_in, key), (value_in, value), (grad_in, grad), (query_in, query), (filt_in, filt),
    )
    loads = [
        pltpu.make_async_copy(
            src.at[:, pl.ds(16 * half, 16)], dst.at[:, pl.ds(16 * half, 16)], load.at[5 * half + k]
        )
        for half in range(2)
        for k, (src, dst) in enumerate(fields)
    ] + [
        pltpu.make_async_copy(src, dst, load.at[10 + k])
        for k, (src, dst) in enumerate(zip(tabs_in, (bias, *tabs)))
    ]
    for copy in loads:
        copy.start()
    barrier = pltpu.get_barrier_semaphore()
    with jax.named_scope("bar_signal"):
        for outer, inner in partners():
            pl.semaphore_signal(
                barrier,
                inc=1,
                device_id={"outer": outer, "inner": inner},
                device_id_type=pl.DeviceIdType.MESH,
            )
    with jax.named_scope("loads"):
        for copy in loads[:5]:
            copy.wait()
    with jax.named_scope("gate0"):
        gate(0, key, value, query, grad, filt, packed)
    with jax.named_scope("bar_wait"):
        pl.semaphore_wait(barrier, DEVICES - 1)
    send_all(packed.at[0], recv.at[0], send_in.at[0], recv_in.at[0], me)
    recv[0, me] = packed[0, me]
    for copy in loads[5:10]:
        copy.wait()
    with jax.named_scope("gate1"):
        gate(1, key, value, query, grad, filt, packed)
    recv[1, me] = packed[1, me]
    with jax.named_scope("sent_in0"):
        wait_all(packed.at[0], send_in.at[0])
    send_all(packed.at[1], recv.at[1], send_in.at[1], recv_in.at[1], me)
    for copy in loads[10:]:
        copy.wait()
    for half in range(2):
        with jax.named_scope(f"wait_in{half}"):
            wait_all(recv.at[half], recv_in.at[half])
        spread(recv.at[half], work)
        with jax.named_scope(f"transforms{half}"):
            run_pairs(work, bias, bias_out, tabs, zf, ff, zi, fi, half)
        gather(work, back.at[half])
        with jax.named_scope(f"send_out{half}"):
            home = early if half == 0 else out
            send_all(back.at[half], home, send_out.at[half], recv_out.at[half], me)
    own = pltpu.make_async_copy(back.at[1, me], out.at[me], own_out)
    own.start()
    early[me] = back[0, me]
    with jax.named_scope("wait_out0"):
        wait_all(early, recv_out.at[0])
    with jax.named_scope("finish0"):
        settle(early, key, value, query, grad, filt)
    wait_all(packed.at[1], send_in.at[1])
    for half in range(2):
        wait_all(back.at[half], send_out.at[half])
    own.wait()
    with jax.named_scope("wait_out1"):
        wait_all(out, recv_out.at[1])


def settle(early, key, value, query, grad, filt):
    @pl.loop(0, DEVICES // 8)
    def _(group):
        at = pl.ds(pl.multiple_of(group * 8, 8), 8)
        rows = (at, slice(0, 16))
        convolved = early[at, :16].astype(F32)
        mixed_grad = early[at, 16:32].astype(F32)
        query[rows] = (query[rows].astype(F32) * convolved).astype(BF)
        grad[rows] = (grad[rows].astype(F32) * convolved).astype(BF)
        value[rows] = (value[rows].astype(F32) * mixed_grad).astype(BF)
        key[rows] = (key[rows].astype(F32) * mixed_grad).astype(BF)
        filt[rows] = early[at, 32:].astype(F32)


def hyena_call(bias, key, value, query, grad, filt):
    consts = [jnp.asarray(t) for t in tables()]
    vmem = pl.BlockSpec(memory_space=pltpu.VMEM)
    hbm = pl.BlockSpec(memory_space=pltpu.HBM)
    rows = jax.ShapeDtypeStruct((DEVICES, 32, 128), BF)
    return pl.pallas_call(
        hyena_kernel,
        out_shape=(
            jax.ShapeDtypeStruct((DEVICES, 48, 128), BF),
            jax.ShapeDtypeStruct((32, 128), F32),
            rows, rows, rows, rows,
            jax.ShapeDtypeStruct((DEVICES, 32, 128), F32),
        ),
        in_specs=[hbm] * 11,
        out_specs=(hbm,) + (vmem,) * 6,
        scratch_shapes=[pltpu.SMEM((1, 32), F32)]
        + [pltpu.VMEM(t.shape, t.dtype) for t in consts]
        + [
            pltpu.VMEM((DEVICES, 48, 128), BF),
            pltpu.VMEM((2, DEVICES, 48, 128), BF),
            pltpu.VMEM((2, DEVICES, 48, 128), BF),
            pltpu.VMEM((2, DEVICES, 48, 128), BF),
            pltpu.VMEM((48 * PITCH, 128), F32),
            pltpu.VMEM((768, 512), BF),
            pltpu.VMEM((768, 256), F32),
            pltpu.VMEM((768, 512), BF),
            pltpu.VMEM((768, 256), F32),
        ]
        + [pltpu.SemaphoreType.DMA((2,))] * 4
        + [pltpu.SemaphoreType.DMA]
        + [pltpu.SemaphoreType.DMA((16,))],
        compiler_params=pltpu.CompilerParams(
            collective_id=0, has_side_effects=True, vmem_limit_bytes=36 * 2**20
        ),
        name="hyena",
    )(
        *[
            pltpu.with_memory_space_constraint(t, pltpu.HBM)
            for t in (key, value, query, grad, filt, bias.reshape(1, 32), *consts)
        ]
    )


def finish_kernel(late, bias_rows, key, value, query, grad, filt, *rest):
    outs, bias_grad, bufs, sems = rest[:5], rest[5], rest[6:11], rest[11]
    first, second = pl.ds(0, 16), pl.ds(16, 16)
    for k, done in enumerate((query, grad, value, key, filt)):
        pltpu.make_async_copy(done.at[:, first], outs[k].at[:, first], sems.at[k]).start()

    @pl.loop(0, DEVICES // BLOCK)
    def _(group):
        at = pl.ds(pl.multiple_of(group * BLOCK, BLOCK), BLOCK)
        convolved = late[at, :16].astype(F32)
        mixed_grad = late[at, 16:32].astype(F32)
        bufs[0][at] = (query[at, second].astype(F32) * convolved).astype(BF)
        bufs[1][at] = (grad[at, second].astype(F32) * convolved).astype(BF)
        bufs[2][at] = (value[at, second].astype(F32) * mixed_grad).astype(BF)
        bufs[3][at] = (key[at, second].astype(F32) * mixed_grad).astype(BF)
        bufs[4][at] = late[at, 32:].astype(F32)
        for k in range(5):
            pltpu.make_async_copy(bufs[k].at[at], outs[k].at[at, second], sems.at[k]).start()

    bias_grad[...] = jnp.sum(bias_rows[...].T, axis=0, keepdims=True)
    for k in range(5):
        pltpu.make_async_copy(outs[k], outs[k], sems.at[k]).wait()


def finish_call(*args):
    vmem = pl.BlockSpec(memory_space=pltpu.VMEM)
    hbm = pl.BlockSpec(memory_space=pltpu.HBM)
    types = (BF, BF, BF, BF, F32)
    return pl.pallas_call(
        finish_kernel,
        out_shape=tuple(jax.ShapeDtypeStruct((DEVICES, 32, 128), t) for t in types)
        + (jax.ShapeDtypeStruct((1, 32), F32),),
        in_specs=[vmem] * 7,
        out_specs=(hbm,) * 5 + (vmem,),
        scratch_shapes=[pltpu.VMEM((DEVICES, 16, 128), t) for t in types]
        + [pltpu.SemaphoreType.DMA((5,))],
        compiler_params=pltpu.CompilerParams(vmem_limit_bytes=16 * 2**20),
        name="finish",
    )(*args)


def on_device(query_gate, key_proj, value_proj, out_grad, filters, skip_bias):
    def rows(array):
        return array.reshape(DEVICES, 32, 128)

    kept = hyena_call(
        skip_bias, rows(key_proj), rows(value_proj), rows(query_gate), rows(out_grad), rows(filters)
    )
    *grads, bias_grad = finish_call(*kept)
    return (*[array.reshape(-1, 128) for array in grads], bias_grad.reshape(-1))


def solution(mesh):
    wide = P(None, AXES)
    return jax.shard_map(
        on_device,
        mesh=mesh,
        in_specs=(wide, wide, wide, wide, wide, P(AXES)),
        out_specs=(wide, wide, wide, wide, wide, P(AXES)),
        check_vma=False,
    )
```

```python
import math, functools
import numpy as np
import jax, jax.numpy as jnp
from jax import lax
from jax.experimental import pallas as pl
from jax.experimental.pallas import tpu as pltpu
from jax.sharding import PartitionSpec as P
BF=jnp.bfloat16; F32=jnp.float32
PITCH=136

def split_np(a):
    hi=np.asarray(a,np.float32).astype(BF)
    lo=(np.asarray(a,np.float64)-np.asarray(hi,np.float64)).astype(np.float32).astype(BF)
    return hi,lo

def tables():
    n=128
    k=np.arange(n)[:,None]; p=np.arange(n)[None,:]
    ang=2*np.pi*((p*(2*k+1))%512)/512
    coarse=np.concatenate([np.cos(ang),-np.sin(ang)],0)
    hi,lo=split_np(coarse)
    fwd_coarse=np.concatenate([hi,lo],1)
    inv=np.concatenate([np.cos(ang),-np.sin(ang)],0).T
    hi,lo=split_np(inv)
    inv_coarse=np.concatenate([hi,lo],1)
    ang=2*np.pi*((k*p)%n)/n
    C,S=np.cos(ang),np.sin(ang)
    fw=np.block([[C,-S],[S,C]])
    iv=np.block([[C,S],[-S,C]])
    hi,lo=split_np(fw); fwd_fine=np.concatenate([hi,lo],0)
    hi,lo=split_np(iv); inv_fine=np.concatenate([hi,lo],0)
    tw=2*np.pi*(p*(2*k+1))/65536.0
    twist=np.concatenate([np.cos(tw),np.sin(tw)],0).astype(np.float32)
    return fwd_coarse,inv_coarse,fwd_fine,inv_fine,twist

def dot(a,b): return jnp.dot(a,b,preferred_element_type=F32)
def split(x):
    hi=x.astype(BF); lo=(x-hi.astype(F32)).astype(BF)
    return hi,lo

def spread(recv, work):
    def body(b,_):
        for u in range(4):
            p=b*4+u
            x=recv[p].astype(F32)
            for j in range(6):
                work[pl.ds(8*j*PITCH+p,8,stride=PITCH),:]=x[8*j:8*j+8]
        return 0
    lax.fori_loop(0,32,body,0)

def gather(work, out):
    def body(b,_):
        for u in range(4):
            p=b*4+u
            x=jnp.concatenate([work[pl.ds(8*j*PITCH+p,8,stride=PITCH),:] for j in range(6)],0)
            out[p]=x.astype(BF)
        return 0
    lax.fori_loop(0,32,body,0)

def run_pairs(work, bias, bias_out, tabs, zf, ff, zi, fi, half):
    fwd_coarse, inv_coarse, fwd_fine, inv_fine, twist = tabs
    tc = twist[:128]
    ts = twist[128:]

    def rows(pair, s, h):
        return pl.ds(pl.multiple_of((s * 16 + 2 * pair + h) * PITCH, 8), 128)

    def put(z, r0, q, value):
        hi, lo = split(value)
        z[r0 : r0 + 128, 128 * q : 128 * q + 128] = hi
        z[r0 : r0 + 128, 256 + 128 * q : 384 + 128 * q] = lo

    def fine(z, f, w, r0, r1):
        zh = z[r0:r1, :256]
        f[r0:r1] = dot(zh, w[:256]) + dot(zh, w[256:]) + dot(z[r0:r1, 256:], w[:256])

    def coarse(pair, s):
        x = jnp.concatenate([work[rows(pair, s, 0), :], work[rows(pair, s, 1), :]], 1).astype(BF)
        return dot(fwd_coarse[...], jnp.concatenate([x, x], 0))

    def turn(s, y):
        for h in range(2):
            yr = y[:128, 128 * h : 128 * h + 128]
            yi = y[128:, 128 * h : 128 * h + 128]
            put(zf, (2 * s + h) * 128, 0, yr * tc + yi * ts)
            put(zf, (2 * s + h) * 128, 1, yi * tc - yr * ts)

    def spectra(s):
        fine(zf, ff, fwd_fine, 2 * s * 128, 2 * s * 128 + 256)

    def products(h):
        mr, mi, gr, gi, fr, fi_ = (
            ff[(2 * s + h) * 128 : (2 * s + h) * 128 + 128, 128 * q : 128 * q + 128]
            for s in range(3)
            for q in range(2)
        )
        for s, pairs in enumerate(
            (
                (mr * fr - mi * fi_, mr * fi_ + mi * fr),
                (gr * fr + gi * fi_, gi * fr - gr * fi_),
                (gr * mr + gi * mi, gi * mr - gr * mi),
            )
        ):
            for q in range(2):
                put(zi, (3 * h + s) * 128, q, pairs[q])

    def back_fine(h):
        fine(zi, fi, inv_fine, 3 * h * 128, 3 * h * 128 + 384)

    def back_turn(s):
        his, los = [], []
        for h in range(2):
            r0 = (3 * h + s) * 128
            ir = fi[r0 : r0 + 128, :128]
            ii = fi[r0 : r0 + 128, 128:]
            rh, rl = split(ir * tc - ii * ts)
            ih, il = split(ii * tc + ir * ts)
            his.append(jnp.concatenate([rh, ih], 0))
            los.append(jnp.concatenate([rl, il], 0))
        return jnp.concatenate(his, 1), jnp.concatenate(los, 1)

    def back_coarse(pair, s, z):
        dh = inv_coarse[:, :256]
        y = dot(dh, z[0]) + dot(inv_coarse[:, 256:], z[0]) + dot(dh, z[1])
        for h in range(2):
            value = y[:, 128 * h : 128 * h + 128] * (1.0 / 16384.0 if s < 2 else 1.0 / 2097152.0)
            channel = half * 16 + 2 * pair + h
            if s < 2:
                own = work[rows(pair, s, h), :]
                if s == 0:
                    bias_out[pl.ds(channel, 1), :] = jnp.sum(
                        own * work[rows(pair, 1, h), :], axis=0, keepdims=True
                    ) * (1.0 / 128.0)
                value = value + bias[0, channel] * own
            work[rows(pair, s, h), :] = value

    for s in range(3):
        turn(s, coarse(0, s))
        spectra(s)

    @pl.loop(0, 7)
    def _(pair):
        y0 = coarse(pair + 1, 0)
        products(0)
        y1 = coarse(pair + 1, 1)
        products(1)
        back_fine(0)
        turn(0, y0)
        y2 = coarse(pair + 1, 2)
        back_fine(1)
        turn(1, y1)
        spectra(0)
        turn(2, y2)
        z0 = back_turn(0)
        spectra(1)
        back_coarse(pair, 0, z0)
        z1 = back_turn(1)
        spectra(2)
        back_coarse(pair, 1, z1)
        back_coarse(pair, 2, back_turn(2))

    for h in range(2):
        products(h)
        back_fine(h)
    for s in range(3):
        back_coarse(7, s, back_turn(s))


AXES = ("outer", "inner")
DEVICES = 128
BLOCK = 16
ORDER = (
    85, 1, 84, 96, 52, 8, 92, 25, 77, 7, 83, 6, 82, 32, 116, 24,
    76, 97, 53, 2, 86, 3, 87, 33, 117, 9, 93, 39, 114, 5, 81, 15,
    91, 17, 69, 40, 124, 10, 95, 102, 51, 34, 119, 11, 94, 31, 75, 26,
    79, 121, 44, 65, 21, 120, 45, 38, 115, 105, 60, 57, 108, 104, 61, 41,
    125, 14, 90, 30, 74, 35, 118, 99, 54, 56, 109, 4, 80, 27, 78, 64,
    20, 16, 68, 98, 55, 103, 50, 127, 42, 46, 122, 37, 113, 22, 67, 100,
    48, 23, 66, 88, 12, 47, 123, 62, 106, 36, 112, 72, 29, 110, 59, 19,
    71, 89, 13, 43, 126, 111, 58, 28, 73, 70, 18, 107, 63, 101, 49,
)


def partners():
    outer = lax.axis_index("outer")
    inner = lax.axis_index("inner")
    z, y, x, core = outer // 2, (inner // 8) * 2 + outer % 2, (inner // 2) % 4, inner % 2
    xs = [(x + k) % 4 for k in range(4)]
    ys = [(y + k) % 4 for k in range(4)]
    zs = [(z + k) % 4 for k in range(4)]
    cores = [(core + k) % 2 for k in range(2)]
    found = []
    for code in ORDER:
        px, pcore = xs[code // 2 % 4], cores[code % 2]
        py, pz = ys[code // 8 % 4], zs[code // 32]
        found.append((pz * 2 + py % 2, (py // 2) * 8 + px * 2 + pcore))
    return found


def send_all(src, dst, send_sem, recv_sem, me):
    for outer, inner in partners():
        pltpu.make_async_remote_copy(
            src_ref=src.at[outer * 16 + inner],
            dst_ref=dst.at[me],
            send_sem=send_sem,
            recv_sem=recv_sem,
            device_id={"outer": outer, "inner": inner},
            device_id_type=pl.DeviceIdType.MESH,
        ).start()


def wait_all(buf, sem):
    rest = buf.at[pl.ds(0, DEVICES - 1)]
    pltpu.make_async_copy(rest, rest, sem).wait()


def gate(half, key, value, query, grad, filt, packed):
    @pl.loop(0, DEVICES // 8)
    def _(group):
        at = (pl.ds(pl.multiple_of(group * 8, 8), 8), pl.ds(16 * half, 16))
        put = packed.at[half, at[0]]
        put[:, :16] = (key[at].astype(F32) * value[at].astype(F32)).astype(BF)
        put[:, 16:32] = (grad[at].astype(F32) * query[at].astype(F32)).astype(BF)
        put[:, 32:] = filt[at].astype(BF)


def hyena_kernel(
    key_in, value_in, query_in, grad_in, filt_in, *rest,
):
    tabs_in, rest = rest[:6], rest[6:]
    out, bias_out, key, value, query, grad, filt = rest[:7]
    tabs, rest = rest[7:13], rest[13:]
    early, packed, recv, back, work, zf, ff, zi, fi, send_in, recv_in, send_out, recv_out, own_out, load = rest
    bias, tabs = tabs[0], tabs[1:]
    me = lax.axis_index("outer") * 16 + lax.axis_index("inner")
    fields = (
        (key_in, key), (value_in, value), (grad_in, grad), (query_in, query), (filt_in, filt),
    )
    loads = [
        pltpu.make_async_copy(
            src.at[:, pl.ds(16 * half, 16)], dst.at[:, pl.ds(16 * half, 16)], load.at[5 * half + k]
        )
        for half in range(2)
        for k, (src, dst) in enumerate(fields)
    ] + [
        pltpu.make_async_copy(src, dst, load.at[10 + k])
        for k, (src, dst) in enumerate(zip(tabs_in, (bias, *tabs)))
    ]
    for copy in loads:
        copy.start()
    barrier = pltpu.get_barrier_semaphore()
    with jax.named_scope("bar_signal"):
        for outer, inner in partners():
            pl.semaphore_signal(
                barrier,
                inc=1,
                device_id={"outer": outer, "inner": inner},
                device_id_type=pl.DeviceIdType.MESH,
            )
    with jax.named_scope("loads"):
        for copy in loads[:5]:
            copy.wait()
    with jax.named_scope("gate0"):
        gate(0, key, value, query, grad, filt, packed)
    with jax.named_scope("bar_wait"):
        pl.semaphore_wait(barrier, DEVICES - 1)
    send_all(packed.at[0], recv.at[0], send_in.at[0], recv_in.at[0], me)
    recv[0, me] = packed[0, me]
    for copy in loads[5:10]:
        copy.wait()
    with jax.named_scope("gate1"):
        gate(1, key, value, query, grad, filt, packed)
    recv[1, me] = packed[1, me]
    with jax.named_scope("sent_in0"):
        wait_all(packed.at[0], send_in.at[0])
    send_all(packed.at[1], recv.at[1], send_in.at[1], recv_in.at[1], me)
    for copy in loads[10:]:
        copy.wait()
    for half in range(2):
        with jax.named_scope(f"wait_in{half}"):
            wait_all(recv.at[half], recv_in.at[half])
        spread(recv.at[half], work)
        with jax.named_scope(f"transforms{half}"):
            run_pairs(work, bias, bias_out, tabs, zf, ff, zi, fi, half)
        gather(work, back.at[half])
        with jax.named_scope(f"send_out{half}"):
            home = early if half == 0 else out
            send_all(back.at[half], home, send_out.at[half], recv_out.at[half], me)
    own = pltpu.make_async_copy(back.at[1, me], out.at[me], own_out)
    own.start()
    early[me] = back[0, me]
    with jax.named_scope("wait_out0"):
        wait_all(early, recv_out.at[0])
    with jax.named_scope("finish0"):
        settle(early, key, value, query, grad, filt)
    wait_all(packed.at[1], send_in.at[1])
    for half in range(2):
        wait_all(back.at[half], send_out.at[half])
    own.wait()
    with jax.named_scope("wait_out1"):
        wait_all(out, recv_out.at[1])


def settle(early, key, value, query, grad, filt):
    @pl.loop(0, DEVICES // 8)
    def _(group):
        at = pl.ds(pl.multiple_of(group * 8, 8), 8)
        rows = (at, slice(0, 16))
        convolved = early[at, :16].astype(F32)
        mixed_grad = early[at, 16:32].astype(F32)
        query[rows] = (query[rows].astype(F32) * convolved).astype(BF)
        grad[rows] = (grad[rows].astype(F32) * convolved).astype(BF)
        value[rows] = (value[rows].astype(F32) * mixed_grad).astype(BF)
        key[rows] = (key[rows].astype(F32) * mixed_grad).astype(BF)
        filt[rows] = early[at, 32:].astype(F32)


def hyena_call(bias, key, value, query, grad, filt):
    consts = [jnp.asarray(t) for t in tables()]
    vmem = pl.BlockSpec(memory_space=pltpu.VMEM)
    hbm = pl.BlockSpec(memory_space=pltpu.HBM)
    rows = jax.ShapeDtypeStruct((DEVICES, 32, 128), BF)
    return pl.pallas_call(
        hyena_kernel,
        out_shape=(
            jax.ShapeDtypeStruct((DEVICES, 48, 128), BF),
            jax.ShapeDtypeStruct((32, 128), F32),
            rows, rows, rows, rows,
            jax.ShapeDtypeStruct((DEVICES, 32, 128), F32),
        ),
        in_specs=[hbm] * 11,
        out_specs=(hbm,) + (vmem,) * 6,
        scratch_shapes=[pltpu.SMEM((1, 32), F32)]
        + [pltpu.VMEM(t.shape, t.dtype) for t in consts]
        + [
            pltpu.VMEM((DEVICES, 48, 128), BF),
            pltpu.VMEM((2, DEVICES, 48, 128), BF),
            pltpu.VMEM((2, DEVICES, 48, 128), BF),
            pltpu.VMEM((2, DEVICES, 48, 128), BF),
            pltpu.VMEM((49 * PITCH, 128), F32),
            pltpu.VMEM((768, 512), BF),
            pltpu.VMEM((768, 256), F32),
            pltpu.VMEM((768, 512), BF),
            pltpu.VMEM((768, 256), F32),
        ]
        + [pltpu.SemaphoreType.DMA((2,))] * 4
        + [pltpu.SemaphoreType.DMA]
        + [pltpu.SemaphoreType.DMA((16,))],
        compiler_params=pltpu.CompilerParams(
            collective_id=0, has_side_effects=True, vmem_limit_bytes=36 * 2**20
        ),
        name="hyena",
    )(
        *[
            pltpu.with_memory_space_constraint(t, pltpu.HBM)
            for t in (key, value, query, grad, filt, bias.reshape(1, 32), *consts)
        ]
    )


def finish_kernel(late, bias_rows, key, value, query, grad, filt, *rest):
    outs, bias_grad, bufs, sems = rest[:5], rest[5], rest[6:11], rest[11]
    first, second = pl.ds(0, 16), pl.ds(16, 16)
    for k, done in enumerate((query, grad, value, key, filt)):
        pltpu.make_async_copy(done.at[:, first], outs[k].at[:, first], sems.at[k]).start()

    @pl.loop(0, DEVICES // BLOCK)
    def _(group):
        at = pl.ds(pl.multiple_of(group * BLOCK, BLOCK), BLOCK)
        convolved = late[at, :16].astype(F32)
        mixed_grad = late[at, 16:32].astype(F32)
        bufs[0][at] = (query[at, second].astype(F32) * convolved).astype(BF)
        bufs[1][at] = (grad[at, second].astype(F32) * convolved).astype(BF)
        bufs[2][at] = (value[at, second].astype(F32) * mixed_grad).astype(BF)
        bufs[3][at] = (key[at, second].astype(F32) * mixed_grad).astype(BF)
        bufs[4][at] = late[at, 32:].astype(F32)
        for k in range(5):
            pltpu.make_async_copy(bufs[k].at[at], outs[k].at[at, second], sems.at[k]).start()

    bias_grad[...] = jnp.sum(bias_rows[...].T, axis=0, keepdims=True)
    for k in range(5):
        pltpu.make_async_copy(outs[k], outs[k], sems.at[k]).wait()


def finish_call(*args):
    vmem = pl.BlockSpec(memory_space=pltpu.VMEM)
    hbm = pl.BlockSpec(memory_space=pltpu.HBM)
    types = (BF, BF, BF, BF, F32)
    return pl.pallas_call(
        finish_kernel,
        out_shape=tuple(jax.ShapeDtypeStruct((DEVICES, 32, 128), t) for t in types)
        + (jax.ShapeDtypeStruct((1, 32), F32),),
        in_specs=[vmem] * 7,
        out_specs=(hbm,) * 5 + (vmem,),
        scratch_shapes=[pltpu.VMEM((DEVICES, 16, 128), t) for t in types]
        + [pltpu.SemaphoreType.DMA((5,))],
        compiler_params=pltpu.CompilerParams(vmem_limit_bytes=16 * 2**20),
        name="finish",
    )(*args)


def on_device(query_gate, key_proj, value_proj, out_grad, filters, skip_bias):
    def rows(array):
        return array.reshape(DEVICES, 32, 128)

    kept = hyena_call(
        skip_bias, rows(key_proj), rows(value_proj), rows(query_gate), rows(out_grad), rows(filters)
    )
    *grads, bias_grad = finish_call(*kept)
    return (*[array.reshape(-1, 128) for array in grads], bias_grad.reshape(-1))


def solution(mesh):
    wide = P(None, AXES)
    return jax.shard_map(
        on_device,
        mesh=mesh,
        in_specs=(wide, wide, wide, wide, wide, P(AXES)),
        out_specs=(wide, wide, wide, wide, wide, P(AXES)),
        check_vma=False,
    )
```

```python
import math, functools
import numpy as np
import jax, jax.numpy as jnp
from jax import lax
from jax.experimental import pallas as pl
from jax.experimental.pallas import tpu as pltpu
from jax.sharding import PartitionSpec as P
BF=jnp.bfloat16; F32=jnp.float32
PITCH=136

def split_np(a):
    hi=np.asarray(a,np.float32).astype(BF)
    lo=(np.asarray(a,np.float64)-np.asarray(hi,np.float64)).astype(np.float32).astype(BF)
    return hi,lo

def tables():
    n=128
    k=np.arange(n)[:,None]; p=np.arange(n)[None,:]
    ang=2*np.pi*((p*(2*k+1))%512)/512
    coarse=np.concatenate([np.cos(ang),-np.sin(ang)],0)
    hi,lo=split_np(coarse)
    fwd_coarse=np.concatenate([hi,lo],1)
    inv=np.concatenate([np.cos(ang),-np.sin(ang)],0).T
    hi,lo=split_np(inv)
    inv_coarse=np.concatenate([hi,lo],1)
    ang=2*np.pi*((k*p)%n)/n
    C,S=np.cos(ang),np.sin(ang)
    fw=np.block([[C,-S],[S,C]])
    iv=np.block([[C,S],[-S,C]])
    hi,lo=split_np(fw); fwd_fine=np.concatenate([hi,lo],0)
    hi,lo=split_np(iv); inv_fine=np.concatenate([hi,lo],0)
    tw=2*np.pi*(p*(2*k+1))/65536.0
    twist=np.concatenate([np.cos(tw),np.sin(tw)],0).astype(np.float32)
    return fwd_coarse,inv_coarse,fwd_fine,inv_fine,twist

def dot(a,b): return jnp.dot(a,b,preferred_element_type=F32)
def split(x):
    hi=x.astype(BF); lo=(x-hi.astype(F32)).astype(BF)
    return hi,lo

def spread(recv, work):
    def body(b,_):
        for u in range(4):
            p=b*4+u
            x=recv[p].astype(F32)
            for j in range(6):
                work[pl.ds(8*j*PITCH+p,8,stride=PITCH),:]=x[8*j:8*j+8]
        return 0
    lax.fori_loop(0,32,body,0)

def gather(work, out):
    def body(b,_):
        for u in range(4):
            p=b*4+u
            x=jnp.concatenate([work[pl.ds(8*j*PITCH+p,8,stride=PITCH),:] for j in range(6)],0)
            out[p]=x.astype(BF)
        return 0
    lax.fori_loop(0,32,body,0)

def run_pairs(work, bias, bias_out, tabs, zf, ff, zi, fi, half):
    fwd_coarse, inv_coarse, fwd_fine, inv_fine, twist = tabs
    tc = twist[:128]
    ts = twist[128:]

    def rows(pair, s, h):
        return pl.ds(pl.multiple_of((s * 16 + 2 * pair + h) * PITCH, 8), 128)

    def put(z, r0, q, value):
        hi, lo = split(value)
        z[r0 : r0 + 128, 128 * q : 128 * q + 128] = hi
        z[r0 : r0 + 128, 256 + 128 * q : 384 + 128 * q] = lo

    def fine(z, f, w, r0, r1):
        zh = z[r0:r1, :256]
        f[r0:r1] = dot(zh, w[:256]) + dot(zh, w[256:]) + dot(z[r0:r1, 256:], w[:256])

    def coarse(pair, s):
        x = jnp.concatenate([work[rows(pair, s, 0), :], work[rows(pair, s, 1), :]], 1).astype(BF)
        return dot(fwd_coarse[...], jnp.concatenate([x, x], 0))

    def turn(s, y):
        for h in range(2):
            yr = y[:128, 128 * h : 128 * h + 128]
            yi = y[128:, 128 * h : 128 * h + 128]
            put(zf, (2 * s + h) * 128, 0, yr * tc + yi * ts)
            put(zf, (2 * s + h) * 128, 1, yi * tc - yr * ts)

    def spectra(s):
        fine(zf, ff, fwd_fine, 2 * s * 128, 2 * s * 128 + 256)

    def products(h):
        mr, mi, gr, gi, fr, fi_ = (
            ff[(2 * s + h) * 128 : (2 * s + h) * 128 + 128, 128 * q : 128 * q + 128]
            for s in range(3)
            for q in range(2)
        )
        for s, pairs in enumerate(
            (
                (mr * fr - mi * fi_, mr * fi_ + mi * fr),
                (gr * fr + gi * fi_, gi * fr - gr * fi_),
                (gr * mr + gi * mi, gi * mr - gr * mi),
            )
        ):
            for q in range(2):
                put(zi, (3 * h + s) * 128, q, pairs[q])

    def back_fine(h):
        fine(zi, fi, inv_fine, 3 * h * 128, 3 * h * 128 + 384)

    def back_turn(s):
        his, los = [], []
        for h in range(2):
            r0 = (3 * h + s) * 128
            ir = fi[r0 : r0 + 128, :128]
            ii = fi[r0 : r0 + 128, 128:]
            rh, rl = split(ir * tc - ii * ts)
            ih, il = split(ii * tc + ir * ts)
            his.append(jnp.concatenate([rh, ih], 0))
            los.append(jnp.concatenate([rl, il], 0))
        return jnp.concatenate(his, 1), jnp.concatenate(los, 1)

    def back_coarse(pair, s, z):
        dh = inv_coarse[:, :256]
        y = dot(dh, z[0]) + dot(inv_coarse[:, 256:], z[0]) + dot(dh, z[1])
        for h in range(2):
            value = y[:, 128 * h : 128 * h + 128] * (1.0 / 16384.0 if s < 2 else 1.0 / 2097152.0)
            channel = half * 16 + 2 * pair + h
            if s < 2:
                own = work[rows(pair, s, h), :]
                if s == 0:
                    bias_out[pl.ds(channel, 1), :] = jnp.sum(
                        own * work[rows(pair, 1, h), :], axis=0, keepdims=True
                    ) * (1.0 / 128.0)
                value = value + bias[0, channel] * own
            work[rows(pair, s, h), :] = value

    for s in range(3):
        turn(s, coarse(0, s))
        spectra(s)

    @pl.loop(0, 7)
    def _(pair):
        y0 = coarse(pair + 1, 0)
        products(0)
        y1 = coarse(pair + 1, 1)
        products(1)
        back_fine(0)
        turn(0, y0)
        y2 = coarse(pair + 1, 2)
        back_fine(1)
        turn(1, y1)
        spectra(0)
        turn(2, y2)
        z0 = back_turn(0)
        spectra(1)
        back_coarse(pair, 0, z0)
        z1 = back_turn(1)
        spectra(2)
        back_coarse(pair, 1, z1)
        back_coarse(pair, 2, back_turn(2))

    for h in range(2):
        products(h)
        back_fine(h)
    for s in range(3):
        back_coarse(7, s, back_turn(s))


AXES = ("outer", "inner")
DEVICES = 128
BLOCK = 16
HEAD = 112
ORDER = (
    85, 1, 84, 96, 52, 8, 92, 25, 77, 7, 83, 6, 82, 32, 116, 24,
    76, 97, 53, 2, 86, 3, 87, 33, 117, 9, 93, 39, 114, 5, 81, 15,
    91, 17, 69, 40, 124, 10, 95, 102, 51, 34, 119, 11, 94, 31, 75, 26,
    79, 121, 44, 65, 21, 120, 45, 38, 115, 105, 60, 57, 108, 104, 61, 41,
    125, 14, 90, 30, 74, 35, 118, 99, 54, 56, 109, 4, 80, 27, 78, 64,
    20, 16, 68, 98, 55, 103, 50, 127, 42, 46, 122, 37, 113, 22, 67, 100,
    48, 23, 66, 88, 12, 47, 123, 62, 106, 36, 112, 72, 29, 110, 59, 19,
    71, 89, 13, 43, 126, 111, 58, 28, 73, 70, 18, 107, 63, 101, 49,
)


def partners():
    outer = lax.axis_index("outer")
    inner = lax.axis_index("inner")
    z, y, x, core = outer // 2, (inner // 8) * 2 + outer % 2, (inner // 2) % 4, inner % 2
    xs = [(x + k) % 4 for k in range(4)]
    ys = [(y + k) % 4 for k in range(4)]
    zs = [(z + k) % 4 for k in range(4)]
    cores = [(core + k) % 2 for k in range(2)]
    found = []
    for code in ORDER:
        px, pcore = xs[code // 2 % 4], cores[code % 2]
        py, pz = ys[code // 8 % 4], zs[code // 32]
        found.append((pz * 2 + py % 2, (py // 2) * 8 + px * 2 + pcore))
    return found


def send_all(src, dst, send_sem, recv_sem, me, tail_sem=None):
    for k, (outer, inner) in enumerate(partners()):
        pltpu.make_async_remote_copy(
            src_ref=src.at[outer * 16 + inner],
            dst_ref=dst.at[me],
            send_sem=send_sem if tail_sem is None or k < HEAD else tail_sem,
            recv_sem=recv_sem,
            device_id={"outer": outer, "inner": inner},
            device_id_type=pl.DeviceIdType.MESH,
        ).start()


def wait_all(buf, sem, count=DEVICES - 1):
    rest = buf.at[pl.ds(0, count)]
    pltpu.make_async_copy(rest, rest, sem).wait()


def gate(half, key, value, query, grad, filt, packed):
    @pl.loop(0, DEVICES // 8)
    def _(group):
        at = (pl.ds(pl.multiple_of(group * 8, 8), 8), pl.ds(16 * half, 16))
        put = packed.at[half, at[0]]
        put[:, :16] = (key[at].astype(F32) * value[at].astype(F32)).astype(BF)
        put[:, 16:32] = (grad[at].astype(F32) * query[at].astype(F32)).astype(BF)
        put[:, 32:] = filt[at].astype(BF)


def hyena_kernel(
    key_in, value_in, query_in, grad_in, filt_in, *rest,
):
    tabs_in, rest = rest[:6], rest[6:]
    out, bias_out, key, value, query, grad, filt = rest[:7]
    tabs, rest = rest[7:13], rest[13:]
    early, packed, recv, back, work, zf, ff, zi, fi, send_in, recv_in, send_out, recv_out, own_out, load = rest
    bias, tabs = tabs[0], tabs[1:]
    me = lax.axis_index("outer") * 16 + lax.axis_index("inner")
    fields = (
        (key_in, key), (value_in, value), (grad_in, grad), (query_in, query), (filt_in, filt),
    )
    loads = [
        pltpu.make_async_copy(
            src.at[:, pl.ds(16 * half, 16)], dst.at[:, pl.ds(16 * half, 16)], load.at[5 * half + k]
        )
        for half in range(2)
        for k, (src, dst) in enumerate(fields)
    ] + [
        pltpu.make_async_copy(src, dst, load.at[10 + k])
        for k, (src, dst) in enumerate(zip(tabs_in, (bias, *tabs)))
    ]
    for copy in loads:
        copy.start()
    barrier = pltpu.get_barrier_semaphore()
    with jax.named_scope("bar_signal"):
        for outer, inner in partners():
            pl.semaphore_signal(
                barrier,
                inc=1,
                device_id={"outer": outer, "inner": inner},
                device_id_type=pl.DeviceIdType.MESH,
            )
    with jax.named_scope("loads"):
        for copy in loads[:5]:
            copy.wait()
    with jax.named_scope("gate0"):
        gate(0, key, value, query, grad, filt, packed)
    with jax.named_scope("bar_wait"):
        pl.semaphore_wait(barrier, DEVICES - 1)
    send_all(packed.at[0], recv.at[0], send_in.at[0], recv_in.at[0], me, send_in.at[2])
    recv[0, me] = packed[0, me]
    for copy in loads[5:10]:
        copy.wait()
    with jax.named_scope("gate1"):
        gate(1, key, value, query, grad, filt, packed)
    recv[1, me] = packed[1, me]
    with jax.named_scope("sent_in0"):
        wait_all(packed.at[0], send_in.at[0], HEAD)
    send_all(packed.at[1], recv.at[1], send_in.at[1], recv_in.at[1], me)
    for copy in loads[10:]:
        copy.wait()
    for half in range(2):
        with jax.named_scope(f"wait_in{half}"):
            wait_all(recv.at[half], recv_in.at[half])
        spread(recv.at[half], work)
        with jax.named_scope(f"transforms{half}"):
            run_pairs(work, bias, bias_out, tabs, zf, ff, zi, fi, half)
        gather(work, back.at[half])
        with jax.named_scope(f"send_out{half}"):
            home = early if half == 0 else out
            send_all(back.at[half], home, send_out.at[half], recv_out.at[half], me)
    own = pltpu.make_async_copy(back.at[1, me], out.at[me], own_out)
    own.start()
    early[me] = back[0, me]
    with jax.named_scope("wait_out0"):
        wait_all(early, recv_out.at[0])
    with jax.named_scope("finish0"):
        settle(early, key, value, query, grad, filt)
    wait_all(packed.at[0], send_in.at[2], DEVICES - 1 - HEAD)
    wait_all(packed.at[1], send_in.at[1])
    for half in range(2):
        wait_all(back.at[half], send_out.at[half])
    own.wait()
    with jax.named_scope("wait_out1"):
        wait_all(out, recv_out.at[1])


def settle(early, key, value, query, grad, filt):
    @pl.loop(0, DEVICES // 8)
    def _(group):
        at = pl.ds(pl.multiple_of(group * 8, 8), 8)
        rows = (at, slice(0, 16))
        convolved = early[at, :16].astype(F32)
        mixed_grad = early[at, 16:32].astype(F32)
        query[rows] = (query[rows].astype(F32) * convolved).astype(BF)
        grad[rows] = (grad[rows].astype(F32) * convolved).astype(BF)
        value[rows] = (value[rows].astype(F32) * mixed_grad).astype(BF)
        key[rows] = (key[rows].astype(F32) * mixed_grad).astype(BF)
        filt[rows] = early[at, 32:].astype(F32)


def hyena_call(bias, key, value, query, grad, filt):
    consts = [jnp.asarray(t) for t in tables()]
    vmem = pl.BlockSpec(memory_space=pltpu.VMEM)
    hbm = pl.BlockSpec(memory_space=pltpu.HBM)
    rows = jax.ShapeDtypeStruct((DEVICES, 32, 128), BF)
    return pl.pallas_call(
        hyena_kernel,
        out_shape=(
            jax.ShapeDtypeStruct((DEVICES, 48, 128), BF),
            jax.ShapeDtypeStruct((32, 128), F32),
            rows, rows, rows, rows,
            jax.ShapeDtypeStruct((DEVICES, 32, 128), F32),
        ),
        in_specs=[hbm] * 11,
        out_specs=(hbm,) + (vmem,) * 6,
        scratch_shapes=[pltpu.SMEM((1, 32), F32)]
        + [pltpu.VMEM(t.shape, t.dtype) for t in consts]
        + [
            pltpu.VMEM((DEVICES, 48, 128), BF),
            pltpu.VMEM((2, DEVICES, 48, 128), BF),
            pltpu.VMEM((2, DEVICES, 48, 128), BF),
            pltpu.VMEM((2, DEVICES, 48, 128), BF),
            pltpu.VMEM((49 * PITCH, 128), F32),
            pltpu.VMEM((768, 512), BF),
            pltpu.VMEM((768, 256), F32),
            pltpu.VMEM((768, 512), BF),
            pltpu.VMEM((768, 256), F32),
        ]
        + [pltpu.SemaphoreType.DMA((3,))] * 4
        + [pltpu.SemaphoreType.DMA]
        + [pltpu.SemaphoreType.DMA((16,))],
        compiler_params=pltpu.CompilerParams(
            collective_id=0, has_side_effects=True, vmem_limit_bytes=36 * 2**20
        ),
        name="hyena",
    )(
        *[
            pltpu.with_memory_space_constraint(t, pltpu.HBM)
            for t in (key, value, query, grad, filt, bias.reshape(1, 32), *consts)
        ]
    )


def finish_kernel(late, bias_rows, key, value, query, grad, filt, *rest):
    outs, bias_grad, bufs, sems = rest[:5], rest[5], rest[6:11], rest[11]
    first, second = pl.ds(0, 16), pl.ds(16, 16)
    for k, done in enumerate((query, grad, value, key, filt)):
        pltpu.make_async_copy(done.at[:, first], outs[k].at[:, first], sems.at[k]).start()

    @pl.loop(0, DEVICES // BLOCK)
    def _(group):
        at = pl.ds(pl.multiple_of(group * BLOCK, BLOCK), BLOCK)
        convolved = late[at, :16].astype(F32)
        mixed_grad = late[at, 16:32].astype(F32)
        bufs[0][at] = (query[at, second].astype(F32) * convolved).astype(BF)
        bufs[1][at] = (grad[at, second].astype(F32) * convolved).astype(BF)
        bufs[2][at] = (value[at, second].astype(F32) * mixed_grad).astype(BF)
        bufs[3][at] = (key[at, second].astype(F32) * mixed_grad).astype(BF)
        bufs[4][at] = late[at, 32:].astype(F32)
        for k in range(5):
            pltpu.make_async_copy(bufs[k].at[at], outs[k].at[at, second], sems.at[k]).start()

    bias_grad[...] = jnp.sum(bias_rows[...].T, axis=0, keepdims=True)
    for k in range(5):
        pltpu.make_async_copy(outs[k], outs[k], sems.at[k]).wait()


def finish_call(*args):
    vmem = pl.BlockSpec(memory_space=pltpu.VMEM)
    hbm = pl.BlockSpec(memory_space=pltpu.HBM)
    types = (BF, BF, BF, BF, F32)
    return pl.pallas_call(
        finish_kernel,
        out_shape=tuple(jax.ShapeDtypeStruct((DEVICES, 32, 128), t) for t in types)
        + (jax.ShapeDtypeStruct((1, 32), F32),),
        in_specs=[vmem] * 7,
        out_specs=(hbm,) * 5 + (vmem,),
        scratch_shapes=[pltpu.VMEM((DEVICES, 16, 128), t) for t in types]
        + [pltpu.SemaphoreType.DMA((5,))],
        compiler_params=pltpu.CompilerParams(vmem_limit_bytes=16 * 2**20),
        name="finish",
    )(*args)


def on_device(query_gate, key_proj, value_proj, out_grad, filters, skip_bias):
    def rows(array):
        return array.reshape(DEVICES, 32, 128)

    kept = hyena_call(
        skip_bias, rows(key_proj), rows(value_proj), rows(query_gate), rows(out_grad), rows(filters)
    )
    *grads, bias_grad = finish_call(*kept)
    return (*[array.reshape(-1, 128) for array in grads], bias_grad.reshape(-1))


def solution(mesh):
    wide = P(None, AXES)
    return jax.shard_map(
        on_device,
        mesh=mesh,
        in_specs=(wide, wide, wide, wide, wide, P(AXES)),
        out_specs=(wide, wide, wide, wide, wide, P(AXES)),
        check_vma=False,
    )
```
